8 devices in a mesh: dp: 1 (over z), sp: 8 (over x, y, core).
Axes of the slice: x: 2, y: 2, z: 1, core: 2. Of those that a mesh axis runs over, the one named last changes fastest.
Arguments:
- x: bfloat16 [2048, 4096], P(('dp', 'sp'))
- gain: bfloat16 [4096], replicated
- wq: bfloat16 [4096, 6144], replicated
- wk: bfloat16 [4096, 1024], replicated
- wv: bfloat16 [4096, 1024], replicated
- wo: bfloat16 [6144, 4096], replicated
Outputs:
- output: bfloat16 [2048, 4096], P(('dp', 'sp'))
All inputs are finite; a program needn't handle non-finite values.
Results may differ from the reference program's by a relative error of at most 0.012.
Values are sent between devices in bfloat16 or wider.
A program may use at most 2 GiB of HBM per device.

```python
import jax
import jax.numpy as jnp
from jax import lax

ROWS = 2048
D = 4096
HEADS = 48
KV_HEADS = 8
HEAD = 128
THETA = 10000


def setup_inputs(seed: int = 0, part: int = 0) -> dict:
    kx, kn, kq, kk, kv, ko = jax.random.split(jax.random.key(seed), 6)

    def weights(key, rows, columns):
        return jax.random.normal(key, (rows, columns), jnp.float32) * rows**-0.5

    drawn = {
        "x": jax.random.normal(jax.random.fold_in(kx, part), (ROWS, D), jnp.float32),
        "gain": 1 + 0.1 * jax.random.normal(kn, (D,), jnp.float32),
        "wq": 2 * weights(kq, D, HEADS * HEAD),
        "wk": 2 * weights(kk, D, KV_HEADS * HEAD),
        "wv": 4 * weights(kv, D, KV_HEADS * HEAD),
        "wo": weights(ko, HEADS * HEAD, D),
    }
    return {k: v.astype(jnp.bfloat16) for k, v in drawn.items()}


def normed(x, gain):
    wide = x.astype(jnp.float32)
    scale = lax.rsqrt(jnp.mean(wide * wide, -1, keepdims=True) + 1e-6)
    return (wide * scale * gain.astype(jnp.float32)).astype(jnp.bfloat16)


def turned(t, place, theta):
    half = t.shape[-1] // 2
    angle = place.astype(jnp.float32)[:, None] * theta ** (-jnp.arange(half, dtype=jnp.float32) / half)
    cos, sin = jnp.cos(angle)[:, None], jnp.sin(angle)[:, None]
    a, b = t[..., :half].astype(jnp.float32), t[..., half:].astype(jnp.float32)
    return jnp.concatenate([a * cos - b * sin, b * cos + a * sin], -1).astype(jnp.bfloat16)


def matmul(a, w):
    return jnp.dot(a, w, preferred_element_type=jnp.float32).astype(jnp.bfloat16)


def einsum(form, a, b):
    return jnp.einsum(form, a.astype(jnp.float32), b.astype(jnp.float32))


def attention(q, k, v):
    scores = einsum("tgsd,ugd->gstu", q, k) * q.shape[-1] ** -0.5
    token = jnp.arange(q.shape[0])
    scores = jnp.where(token[:, None] >= token, scores, -jnp.inf)
    weights = jax.nn.softmax(scores, -1).astype(jnp.bfloat16)
    return einsum("gstu,ugd->tgsd", weights, v).astype(jnp.bfloat16)


def reference(x, gain, wq, wk, wv, wo):
    a, place = normed(x, gain), jnp.arange(ROWS)
    q = turned(matmul(a, wq).reshape(ROWS, HEADS, HEAD), place, THETA).reshape(ROWS, KV_HEADS, -1, HEAD)
    k = turned(matmul(a, wk).reshape(ROWS, KV_HEADS, HEAD), place, THETA)
    v = matmul(a, wv).reshape(ROWS, KV_HEADS, HEAD)
    seen = attention(q, k, v).reshape(ROWS, HEADS * HEAD)
    return (x.astype(jnp.float32) + jnp.dot(seen, wo, preferred_element_type=jnp.float32)).astype(jnp.bfloat16)
```

```python
import functools

import numpy as np
import jax
import jax.numpy as jnp
from jax import lax
from jax.experimental import pallas as pl
from jax.experimental.pallas import tpu as pltpu
from jax.sharding import PartitionSpec as P

HEAD = 128
THETA = 10000
HIDDEN = -2e30
LOG2E = 1.4426950408889634
E2 = HEAD**-0.5 * LOG2E
MESH = pl.DeviceIdType.MESH
CHIPS = 4
SLOTS = 6


def _dot(a, b, ca, cb):
    return lax.dot_general(a, b, (((ca,), (cb,)), ((), ())), preferred_element_type=jnp.float32)


def _tables(rows):
    half = HEAD // 2
    angle = np.arange(rows, dtype=np.float32)[:, None] * np.float32(THETA) ** (-np.arange(half, dtype=np.float32) / np.float32(half))
    angle = angle.astype(np.float32).astype(np.float64)
    return np.concatenate([np.cos(angle), np.sin(angle)], -1).astype(np.float32)


def _attend_full(k, vt, q_ref, heads, top_s, mix_s):
    scores = [_dot(k, q_ref[h], 1, 1) for h in heads]
    weights, keeps = [], []
    for h, s in zip(heads, scores):
        old = top_s[h]
        top = jnp.maximum(old, s.max(axis=0, keepdims=True))
        top_s[h] = top
        weights.append(jnp.exp2((s - top) * E2).astype(jnp.bfloat16))
        keeps.append(jnp.exp2((old - top) * E2))
    for h, p, keep in zip(heads, weights, keeps):
        mix_s[h] = mix_s[h] * keep + _dot(vt, p, 1, 0)


def _attend_own(k_ref, v_ref, q_ref, heads, top_s, mix_s, gap_s, half):
    seen = gap_s[...] >= 0
    scores = []
    for h in heads:
        low = _dot(k_ref[:half], q_ref[h, :half], 1, 1)
        high = _dot(k_ref[...], q_ref[h, half:], 1, 1)
        scores.append((low, high))
    weights = []
    for h, (low, high) in zip(heads, scores):
        low = jnp.where(seen, low, HIDDEN)
        high = jnp.concatenate([high[:half], jnp.where(seen, high[half:], HIDDEN)], axis=0)
        top0, top1 = low.max(axis=0, keepdims=True), high.max(axis=0, keepdims=True)
        top_s[h, :, :half] = top0
        top_s[h, :, half:] = top1
        weights.append((jnp.exp2((low - top0) * E2).astype(jnp.bfloat16), jnp.exp2((high - top1) * E2).astype(jnp.bfloat16)))
    for h, (p0, p1) in zip(heads, weights):
        mix_s[h, :, :half] = _dot(v_ref[:, :half], p0, 1, 0)
        mix_s[h, :, half:] = _dot(v_ref[...], p1, 1, 0)


def _body(x_hbm, gain_ref, wq_hbm, wk_hbm, wv_hbm, tab_hbm, out_hbm, a_s, w_s, k_s, v_s, q_s, top_s, mix_s, seen_s, gap_s, cos_s, sin_s,
          x_sem, w_sem, tab_sem, xs_sem, xr_sem, send_sem, recv_sem, out_sem, os_sem, or_sem):
    own, depth = x_hbm.shape
    tokens = 2 * own
    kv, group = k_s.shape[1], q_s.shape[0] // k_s.shape[1]
    wide = w_s.shape[2]
    per = wide // HEAD
    qcols, kvcols = q_s.shape[0] * HEAD, kv * HEAD
    nq, nk = qcols // wide, kvcols // wide
    me = lax.axis_index("sp")
    chip, core = me // 2, me % 2
    mate = chip * 2 + 1 - core

    def weights(ref, first, i, slot):
        at = pl.multiple_of(core * first + i * wide, wide)
        return pltpu.make_async_copy(ref.at[:, pl.ds(at, wide)], w_s.at[slot], w_sem.at[slot])

    def queries(i):
        return weights(wq_hbm, qcols, i, lax.rem(i + 2 * nk, SLOTS))

    mine = pltpu.make_async_copy(x_hbm, a_s.at[core], x_sem)
    mine.start()
    for i in range(nk):
        weights(wk_hbm, kvcols, i, i).start()
    for i in range(nk):
        weights(wv_hbm, kvcols, i, nk + i).start()
    table = pltpu.make_async_copy(tab_hbm.at[pl.ds(pl.multiple_of(chip * tokens, tokens), tokens)], cos_s, tab_sem)
    table.start()
    for i in range(SLOTS - 2 * nk):
        queries(i).start()

    barrier = pltpu.get_barrier_semaphore()
    pl.semaphore_signal(barrier, inc=1, device_id={"sp": mate}, device_id_type=MESH)
    for r in (1, 2, 3):
        pl.semaphore_signal(barrier, inc=1, device_id={"sp": (chip ^ r) * 2 + core}, device_id_type=MESH)
    pl.semaphore_wait(barrier, 4)

    give = pltpu.make_async_remote_copy(src_ref=x_hbm, dst_ref=a_s.at[core], send_sem=xs_sem, recv_sem=xr_sem, device_id={"sp": mate},
                                        device_id_type=MESH)
    give.start()

    gap_s[...] = lax.broadcasted_iota(jnp.int32, gap_s.shape, 1) - lax.broadcasted_iota(jnp.int32, gap_s.shape, 0)
    v_s[:, :, HEAD:, :] = jnp.ones((*v_s.shape[:2], v_s.shape[2] - HEAD, v_s.shape[3]), jnp.bfloat16)
    table.wait()
    both = cos_s[...]
    turn = pltpu.roll(both, HEAD // 2, 1)
    left = lax.broadcasted_iota(jnp.int32, both.shape, 1) < HEAD // 2
    cos_s[...] = jnp.where(left, both, turn)
    sin_s[...] = jnp.where(left, -turn, both)

    def turned(t, rows):
        t = t.astype(jnp.float32)
        return (t * cos_s[rows, :] + pltpu.roll(t, HEAD // 2, 1) * sin_s[rows, :]).astype(jnp.bfloat16)

    def normed(slot):
        slab = 32

        def one(i, _):
            rows = pl.ds(pl.multiple_of(i * slab, slab), slab)
            t = a_s[slot, rows, :].astype(jnp.float32)
            t = t * lax.rsqrt(jnp.mean(t * t, -1, keepdims=True) + 1e-6) * gain_ref[...].astype(jnp.float32)
            a_s[slot, rows, :] = t.astype(jnp.bfloat16)
            return 0

        lax.fori_loop(0, own // slab, one, 0)

    def keys(slot, first):
        rows = pl.ds(pl.multiple_of(slot * own, own), own)
        for i in range(nk):
            if first:
                weights(wk_hbm, kvcols, i, i).wait()
            t = _dot(a_s[slot], w_s[i], 1, 0).astype(jnp.bfloat16)
            for j in range(per):
                k_s[chip, i * per + j, rows, :] = turned(t[:, j * HEAD : (j + 1) * HEAD], rows)

    def values(slot, first):
        rows = pl.ds(pl.multiple_of(slot * own, own), own)
        for i in range(nk):
            if first:
                weights(wv_hbm, kvcols, i, nk + i).wait()
            t = _dot(a_s[slot], w_s[nk + i], 1, 0)
            for j in range(per):
                v_s[chip, i * per + j, :HEAD, rows] = t[:, j * HEAD : (j + 1) * HEAD].T.astype(jnp.bfloat16)

    mine.wait()
    normed(core)
    keys(core, True)
    values(core, True)
    give.wait_recv()
    normed(1 - core)
    keys(1 - core, False)
    values(1 - core, False)

    def sent(r, what):
        here = k_s.at[chip] if what == 0 else v_s.at[chip, :, pl.ds(0, HEAD), :]
        return pltpu.make_async_remote_copy(src_ref=here, dst_ref=here, send_sem=send_sem.at[r, what], recv_sem=recv_sem.at[chip, what],
                                            device_id={"sp": (chip ^ r) * 2 + core}, device_id_type=MESH)

    def got(r, what):
        there = chip ^ r
        here = k_s.at[there] if what == 0 else v_s.at[there, :, pl.ds(0, HEAD), :]
        return pltpu.make_async_remote_copy(src_ref=here, dst_ref=here, send_sem=send_sem.at[r, what], recv_sem=recv_sem.at[there, what],
                                            device_id={"sp": there * 2 + core}, device_id_type=MESH)

    def send(r, what):
        @pl.when((chip ^ r) > chip)
        def _():
            sent(r, what).start()

    def project(i):
        queries(i).wait()
        slot = lax.rem(i + 2 * nk, SLOTS)
        t = _dot(a_s[...].reshape(tokens, depth), w_s[slot], 1, 0).astype(jnp.bfloat16)
        for j in range(per):
            q_s[i * per + j] = turned(t[:, j * HEAD : (j + 1) * HEAD], slice(None))

        @pl.when(i + SLOTS < nq)
        def _():
            queries(i + SLOTS).start()

    for i in range(SLOTS - 2 * nk, min(SLOTS, nq)):
        queries(i).start()
    send(1, 0)
    send(2, 0)
    lax.fori_loop(0, 1, lambda i, _: (project(i), 0)[1], 0)
    send(1, 1)
    send(2, 1)
    send(3, 0)
    send(3, 1)
    lax.fori_loop(1, nq, lambda i, _: (project(i), 0)[1], 0)

    def first(n, _):
        _attend_own(k_s.at[chip, n], v_s.at[chip, n], q_s, [n * group + j for j in range(group)], top_s, mix_s, gap_s, own)
        return 0

    lax.fori_loop(0, kv, first, 0)

    for r in (1, 2, 3):
        there = chip ^ r

        @pl.when(there < chip)
        def _():
            got(r, 0).wait_recv()
            got(r, 1).wait_recv()

            def more(n, _):
                _attend_full(k_s[there, n], v_s[there, n], q_s, [n * group + j for j in range(group)], top_s, mix_s)
                return 0

            lax.fori_loop(0, kv, more, 0)

    def finish(n, _):
        for j in range(group):
            h = n * group + j
            t = mix_s[h, :HEAD, :] * (1 / mix_s[h, HEAD : HEAD + 1, :])
            seen_s[:, pl.ds(pl.multiple_of(h * HEAD, HEAD), HEAD)] = t.T.astype(jnp.bfloat16)
        return 0

    lax.fori_loop(0, kv, finish, 0)

    columns = pl.ds(pl.multiple_of(core * qcols, qcols), qcols)
    keep = pltpu.make_async_copy(seen_s.at[pl.ds(pl.multiple_of(core * own, own), own), :], out_hbm.at[:, columns], out_sem)
    keep.start()
    back = pltpu.make_async_remote_copy(src_ref=seen_s.at[pl.ds(pl.multiple_of((1 - core) * own, own), own), :], dst_ref=out_hbm.at[:, columns],
                                        send_sem=os_sem, recv_sem=or_sem, device_id={"sp": mate}, device_id_type=MESH)
    back.start()
    for r in (1, 2, 3):
        @pl.when((chip ^ r) > chip)
        def _():
            sent(r, 0).wait_send()
            sent(r, 1).wait_send()
    give.wait_send()
    keep.wait()
    back.wait()


def _seen(x, gain, wq, wk, wv):
    own, depth = x.shape
    tokens, heads, kv = 2 * own, wq.shape[1] // HEAD // 2, wk.shape[1] // HEAD // 2
    wide, bf, f32 = 256, jnp.bfloat16, jnp.float32
    table = jnp.asarray(_tables(tokens * CHIPS))
    hbm = pl.BlockSpec(memory_space=pl.ANY)
    dma = pltpu.SemaphoreType.DMA
    return pl.pallas_call(
        _body,
        out_shape=jax.ShapeDtypeStruct((own, 2 * heads * HEAD), bf),
        in_specs=[hbm, pl.BlockSpec(memory_space=pltpu.VMEM), hbm, hbm, hbm, hbm],
        out_specs=hbm,
        scratch_shapes=[
            pltpu.VMEM((2, own, depth), bf),
            pltpu.VMEM((SLOTS, depth, wide), bf),
            pltpu.VMEM((CHIPS, kv, tokens, HEAD), bf),
            pltpu.VMEM((CHIPS, kv, HEAD + 16, tokens), bf),
            pltpu.VMEM((heads, tokens, HEAD), bf),
            pltpu.VMEM((heads, 1, tokens), f32),
            pltpu.VMEM((heads, HEAD + 16, tokens), f32),
            pltpu.VMEM((tokens, heads * HEAD), bf),
            pltpu.VMEM((own, own), jnp.int32),
            pltpu.VMEM((tokens, HEAD), f32),
            pltpu.VMEM((tokens, HEAD), f32),
            dma, dma((SLOTS,)), dma, dma, dma, dma((CHIPS, 2)), dma((CHIPS, 2)), dma, dma, dma,
        ],
        compiler_params=pltpu.CompilerParams(collective_id=0, has_side_effects=True, vmem_limit_bytes=60 * 2**20),
        name="seen",
    )(x, gain.reshape(1, depth), wq, wk, wv, table)


def _out_body(seen_ref, wo_ref, x_ref, y_ref):
    y = jnp.dot(seen_ref[...], wo_ref[...], preferred_element_type=jnp.float32)
    y_ref[...] = (x_ref[...].astype(jnp.float32) + y).astype(jnp.bfloat16)


def _out(seen, wo, x):
    own, depth = seen.shape
    width, wide = wo.shape[1], 256
    return pl.pallas_call(
        _out_body,
        out_shape=jax.ShapeDtypeStruct((own, width), jnp.bfloat16),
        grid=(width // wide,),
        in_specs=[pl.BlockSpec((own, depth), lambda i: (0, 0)), pl.BlockSpec((depth, wide), lambda i: (0, i)),
                  pl.BlockSpec((own, wide), lambda i: (0, i))],
        out_specs=pl.BlockSpec((own, wide), lambda i: (0, i)),
        compiler_params=pltpu.CompilerParams(dimension_semantics=("arbitrary",), vmem_limit_bytes=48 * 2**20),
        name="out",
    )(seen, wo, x)


def solution(mesh):
    def step(x, gain, wq, wk, wv, wo):
        return _out(_seen(x, gain, wq, wk, wv), wo, x)

    tokens, whole = P(("dp", "sp"), None), P(None, None)
    return jax.shard_map(
        step,
        mesh=mesh,
        in_specs=(tokens, P(None), whole, whole, whole, whole),
        out_specs=tokens,
        check_vma=False,
    )
```

```python
import functools

import numpy as np
import jax
import jax.numpy as jnp
from jax import lax
from jax.experimental import pallas as pl
from jax.experimental.pallas import tpu as pltpu
from jax.sharding import PartitionSpec as P

HEAD = 128
THETA = 10000
HIDDEN = -2e30
LOG2E = 1.4426950408889634
E2 = HEAD**-0.5 * LOG2E
MESH = pl.DeviceIdType.MESH
CHIPS = 4
SLOTS = 6


def _dot(a, b, ca, cb):
    return lax.dot_general(a, b, (((ca,), (cb,)), ((), ())), preferred_element_type=jnp.float32)


def _tables(rows):
    half = HEAD // 2
    angle = np.arange(rows, dtype=np.float32)[:, None] * np.float32(THETA) ** (-np.arange(half, dtype=np.float32) / np.float32(half))
    angle = angle.astype(np.float32).astype(np.float64)
    return np.concatenate([np.cos(angle), np.sin(angle)], -1).astype(np.float32)


def _attend_full(k, vt, q_ref, heads, top_s, mix_s):
    scores = [_dot(k, q_ref[h], 1, 1) for h in heads]
    weights, keeps = [], []
    for h, s in zip(heads, scores):
        old = top_s[h]
        top = jnp.maximum(old, s.max(axis=0, keepdims=True))
        top_s[h] = top
        weights.append(jnp.exp2((s - top) * E2).astype(jnp.bfloat16))
        keeps.append(jnp.exp2((old - top) * E2))
    for h, p, keep in zip(heads, weights, keeps):
        mix_s[h] = mix_s[h] * keep + _dot(vt, p, 1, 0)


def _attend_own(k_ref, v_ref, q_ref, heads, top_s, mix_s, gap_s, half):
    seen = gap_s[...] >= 0
    scores = []
    for h in heads:
        low = _dot(k_ref[:half], q_ref[h, :half], 1, 1)
        high = _dot(k_ref[...], q_ref[h, half:], 1, 1)
        scores.append((low, high))
    weights = []
    for h, (low, high) in zip(heads, scores):
        low = jnp.where(seen, low, HIDDEN)
        high = jnp.concatenate([high[:half], jnp.where(seen, high[half:], HIDDEN)], axis=0)
        top0, top1 = low.max(axis=0, keepdims=True), high.max(axis=0, keepdims=True)
        top_s[h, :, :half] = top0
        top_s[h, :, half:] = top1
        weights.append((jnp.exp2((low - top0) * E2).astype(jnp.bfloat16), jnp.exp2((high - top1) * E2).astype(jnp.bfloat16)))
    for h, (p0, p1) in zip(heads, weights):
        mix_s[h, :, :half] = _dot(v_ref[:, :half], p0, 1, 0)
        mix_s[h, :, half:] = _dot(v_ref[...], p1, 1, 0)


def _body(x_hbm, gain_ref, wq_hbm, wk_hbm, wv_hbm, wo_hbm, tab_hbm, y_hbm, a_s, w_s, k_s, v_s, km_s, vm_s, q_s, top_s, mix_s, own_s, give_s, got_s,
          acc_s, y_s, gap_s, cos_s, sin_s, x_sem, w_sem, tab_sem, xs_sem, xr_sem, mate_send, send_sem, recv_sem, fsend_sem, frecv_sem,
          swap_send, swap_recv, y_sem):
    own, depth = x_hbm.shape
    tokens = 2 * own
    kv, group = k_s.shape[1], q_s.shape[0] // k_s.shape[1]
    wide = w_s.shape[2]
    per = wide // HEAD
    qcols, kvcols = q_s.shape[0] * HEAD, kv * HEAD
    nq, nkv, pieces = qcols // wide, 4 * kvcols // wide, kv // per
    no = depth // wide
    me = lax.axis_index("sp")
    chip, core = me // 2, me % 2
    mate = chip * 2 + 1 - core
    mine = pl.ds(pl.multiple_of(core * own, own), own)

    plan = [(what, half, p) for p in range(pieces) for half in (1, 0) for what in (0, 1)]

    def kv_block(i):
        what, half, p = plan[i]
        at = pl.multiple_of(lax.rem(core + half, 2) * kvcols + p * wide, wide)
        ref = wk_hbm if what == 0 else wv_hbm
        return pltpu.make_async_copy(ref.at[:, pl.ds(at, wide)], w_s.at[i % SLOTS], w_sem.at[i % SLOTS])

    def q_block(i):
        slot = lax.rem(i + nkv, SLOTS)
        at = pl.multiple_of(core * qcols + i * wide, wide)
        return pltpu.make_async_copy(wq_hbm.at[:, pl.ds(at, wide)], w_s.at[slot], w_sem.at[slot])

    def o_block(i):
        slot = lax.rem(i + nkv + nq, SLOTS)
        rows = pl.multiple_of(jnp.where(i < no, core, 1 - core) * qcols, qcols)
        at = pl.multiple_of(lax.rem(i, no) * wide, wide)
        return pltpu.make_async_copy(wo_hbm.at[pl.ds(rows, qcols), pl.ds(at, wide)], w_s.at[slot, pl.ds(0, qcols), :], w_sem.at[slot])

    load = pltpu.make_async_copy(x_hbm, a_s.at[core], x_sem)
    load.start()
    for i in range(SLOTS):
        kv_block(i).start()
    table = pltpu.make_async_copy(tab_hbm.at[pl.ds(pl.multiple_of(chip * tokens, tokens), tokens)], cos_s, tab_sem)
    table.start()

    barrier = pltpu.get_barrier_semaphore()
    pl.semaphore_signal(barrier, inc=1, device_id={"sp": mate}, device_id_type=MESH)
    for r in (1, 2):
        for g in (0, 1):
            pl.semaphore_signal(barrier, inc=1, device_id={"sp": (chip ^ r) * 2 + g}, device_id_type=MESH)
    pl.semaphore_wait(barrier, 5)

    give = pltpu.make_async_remote_copy(src_ref=x_hbm, dst_ref=a_s.at[core], send_sem=xs_sem, recv_sem=xr_sem, device_id={"sp": mate},
                                        device_id_type=MESH)
    give.start()

    gap_s[...] = lax.broadcasted_iota(jnp.int32, gap_s.shape, 1) - lax.broadcasted_iota(jnp.int32, gap_s.shape, 0)
    v_s[:, :, HEAD:, :] = jnp.ones((*v_s.shape[:2], v_s.shape[2] - HEAD, v_s.shape[3]), jnp.bfloat16)
    table.wait()
    both = cos_s[...]
    turn = pltpu.roll(both, HEAD // 2, 1)
    left = lax.broadcasted_iota(jnp.int32, both.shape, 1) < HEAD // 2
    cos_s[...] = jnp.where(left, both, turn)
    sin_s[...] = jnp.where(left, -turn, both)

    def turned(t, rows):
        t = t.astype(jnp.float32)
        return (t * cos_s[rows, :] + pltpu.roll(t, HEAD // 2, 1) * sin_s[rows, :]).astype(jnp.bfloat16)

    def normed(slot, keep):
        slab = 16

        def one(i, _):
            rows = pl.ds(pl.multiple_of(i * slab, slab), slab)
            t = a_s[slot, rows, :].astype(jnp.float32)
            if keep:
                acc_s[rows, :] = t
            t = t * lax.rsqrt(jnp.mean(t * t, -1, keepdims=True) + 1e-6) * gain_ref[...].astype(jnp.float32)
            a_s[slot, rows, :] = t.astype(jnp.bfloat16)
            return 0

        lax.fori_loop(0, own // slab, one, 0)

    def places(what, half, p):
        heads = pl.ds(p * per, per)
        there = k_s.at[chip, heads, mine, :] if what == 0 else v_s.at[chip, heads, pl.ds(0, HEAD), mine]
        if half == 0:
            return there, there
        return (km_s if what == 0 else vm_s).at[heads], there

    def to_mate(what, p):
        src, dst = places(what, 1, p)
        return pltpu.make_async_remote_copy(src_ref=src, dst_ref=dst, send_sem=mate_send.at[what, p], recv_sem=recv_sem.at[chip, core, what, p],
                                            device_id={"sp": mate}, device_id_type=MESH)

    def to_chip(r, what, half, p):
        src, dst = places(what, half, p)
        return pltpu.make_async_remote_copy(src_ref=src, dst_ref=dst, send_sem=send_sem.at[r, what, half, p],
                                            recv_sem=recv_sem.at[chip, core, what, p],
                                            device_id={"sp": (chip ^ r) * 2 + lax.rem(core + half, 2)}, device_id_type=MESH)

    def arrived(there, by, p):
        heads, rows = pl.ds(p * per, per), pl.ds(pl.multiple_of(by * own, own), own)
        for what, ref in ((0, k_s.at[there, heads, rows, :]), (1, v_s.at[there, heads, pl.ds(0, HEAD), rows])):
            pltpu.make_async_remote_copy(src_ref=ref, dst_ref=ref, send_sem=mate_send.at[what, p], recv_sem=recv_sem.at[there, by, what, p],
                                         device_id={"sp": mate}, device_id_type=MESH).wait_recv()

    def passed(source, target, what, p):
        heads = pl.ds(p * per, per)
        ref = k_s.at[source, heads] if what == 0 else v_s.at[source, heads, pl.ds(0, HEAD), :]
        return pltpu.make_async_remote_copy(src_ref=ref, dst_ref=ref, send_sem=fsend_sem.at[what, p], recv_sem=frecv_sem.at[what, p],
                                            device_id={"sp": target * 2 + core}, device_id_type=MESH)

    relay = [(lax.rem(chip, 2) == 1, (chip - 1) // 2, 3 - (chip - 1) // 2), (chip >= 2, chip - 2, 5 - chip)]

    def from_near(p):
        for r in (1, 2):
            @pl.when((chip ^ r) < chip)
            def _():
                arrived(chip ^ r, 0, p)
                arrived(chip ^ r, 1, p)
        does, source, target = relay[p]

        @pl.when(does)
        def _():
            for what in (0, 1):
                passed(source, target, what, p).start()

    def send(i):
        what, half, p = plan[i]
        if half:
            to_mate(what, p).start()
        for r in (1, 2):
            @pl.when((chip ^ r) > chip)
            def _():
                to_chip(r, what, half, p).start()

    load.wait()
    normed(core, True)
    for i in range(nkv):
        what, half, p = plan[i]
        kv_block(i).wait()
        t = _dot(a_s[core], w_s[i % SLOTS], 1, 0)
        for j in range(per):
            u = t[:, j * HEAD : (j + 1) * HEAD]
            n = p * per + j
            if what == 0:
                u = turned(u.astype(jnp.bfloat16), mine)
                if half:
                    km_s[n] = u
                else:
                    k_s[chip, n, mine, :] = u
            else:
                u = u.T.astype(jnp.bfloat16)
                if half:
                    vm_s[n] = u
                else:
                    v_s[chip, n, :HEAD, mine] = u
        if i + SLOTS < nkv:
            kv_block(i + SLOTS).start()
        else:
            q_block(i + SLOTS - nkv).start()
        if i:
            send(i - 1)
    give.wait_recv()
    normed(1 - core, False)
    send(nkv - 1)

    def project(trip, _):
        for j in (0, 1):
            q_block(2 * trip + j).wait()
        for j in (0, 1):
            i = 2 * trip + j
            t = _dot(a_s[...].reshape(tokens, depth), w_s[lax.rem(i + nkv, SLOTS)], 1, 0).astype(jnp.bfloat16)
            for m in range(per):
                q_s[i * per + m] = turned(t[:, m * HEAD : (m + 1) * HEAD], slice(None))
        for j in (0, 1):
            i = 2 * trip + j + SLOTS

            @pl.when(i < nq)
            def _():
                q_block(i).start()

            @pl.when(i >= nq)
            def _():
                o_block(i - nq).start()
        return 0

    lax.fori_loop(0, 4, project, 0)
    from_near(0)
    lax.fori_loop(4, nq // 2, project, 0)

    for p in range(pieces):
        arrived(chip, 1 - core, p)

    def first(n, _):
        _attend_own(k_s.at[chip, n], v_s.at[chip, n], q_s, [n * group + j for j in range(group)], top_s, mix_s, gap_s, own)
        return 0

    lax.fori_loop(0, kv, first, 0)
    from_near(1)

    for r in (1, 2, 3):
        there = chip ^ r

        @pl.when(there < chip)
        def _():
            if r == 3:
                @pl.when(chip >= 2)
                def _():
                    for p in range(pieces):
                        for what in (0, 1):
                            passed(there, chip, what, p).wait_recv()

            def more(n, _):
                _attend_full(k_s[there, n], v_s[there, n], q_s, [n * group + j for j in range(group)], top_s, mix_s)
                return 0

            lax.fori_loop(0, kv, more, 0)

    def swap(n):
        columns = pl.ds(pl.multiple_of(n * group * HEAD, HEAD), group * HEAD)
        return pltpu.make_async_remote_copy(src_ref=give_s.at[:, columns], dst_ref=got_s.at[:, columns], send_sem=swap_send.at[n],
                                            recv_sem=swap_recv.at[n], device_id={"sp": mate}, device_id_type=MESH)

    def finish(n, _):
        for j in range(group):
            h = n * group + j
            column = pl.ds(pl.multiple_of(h * HEAD, HEAD), HEAD)
            for part, ref in ((core, own_s), (1 - core, give_s)):
                lanes = pl.ds(pl.multiple_of(part * own, own), own)
                t = mix_s[h, :HEAD, lanes] * (1 / mix_s[h, HEAD : HEAD + 1, lanes])
                ref[:, column] = t.T.astype(jnp.bfloat16)

        @pl.when(n > 0)
        def _():
            swap(n - 1).start()
        return 0

    lax.fori_loop(0, kv, finish, 0)

    def out(trip, second):
        for j in (0, 1):
            o_block(2 * trip + j).wait()
        for j in (0, 1):
            i = 2 * trip + j
            column = pl.ds(pl.multiple_of(lax.rem(i, no) * wide, wide), wide)
            t = acc_s[:, column] + _dot((got_s if second else own_s)[...], w_s[lax.rem(i + nkv + nq, SLOTS), :qcols, :], 1, 0)
            if second:
                y_s[:, column] = t.astype(jnp.bfloat16)
            else:
                acc_s[:, column] = t
        for j in (0, 1):
            i = 2 * trip + j + SLOTS

            @pl.when(i < 2 * no)
            def _():
                o_block(i).start()

    def result(i):
        column = pl.ds(pl.multiple_of(i * 2 * wide, wide), 2 * wide)
        return pltpu.make_async_copy(y_s.at[:, column], y_hbm.at[:, column], y_sem.at[i])

    def out_own(trip, _):
        out(trip, False)

        @pl.when(trip == 0)
        def _():
            swap(kv - 1).start()
        return 0

    lax.fori_loop(0, no // 2, out_own, 0)
    for n in range(kv):
        swap(n).wait_recv()

    def out_mate(trip, _):
        out(trip, True)

        @pl.when(trip > no // 2)
        def _():
            result(trip - no // 2 - 1).start()
        return 0

    lax.fori_loop(no // 2, no, out_mate, 0)
    result(no // 2 - 1).start()

    for p in range(pieces):
        for what in (0, 1):
            to_mate(what, p).wait_send()
    for r in (1, 2):
        @pl.when((chip ^ r) > chip)
        def _():
            for what, half, p in plan:
                to_chip(r, what, half, p).wait_send()
    for p in range(pieces):
        does, source, target = relay[p]

        @pl.when(does)
        def _():
            for what in (0, 1):
                passed(source, target, what, p).wait_send()
    for n in range(kv):
        swap(n).wait_send()
    give.wait_send()
    for i in range(no // 2):
        result(i).wait()


def _program(x, gain, wq, wk, wv, wo):
    own, depth = x.shape
    tokens, heads, kv = 2 * own, wq.shape[1] // HEAD // 2, wk.shape[1] // HEAD // 2
    wide, bf, f32 = 256, jnp.bfloat16, jnp.float32
    table = jnp.asarray(_tables(tokens * CHIPS))
    hbm = pl.BlockSpec(memory_space=pl.ANY)
    dma = pltpu.SemaphoreType.DMA
    return pl.pallas_call(
        _body,
        out_shape=jax.ShapeDtypeStruct((own, depth), bf),
        in_specs=[hbm, pl.BlockSpec(memory_space=pltpu.VMEM), hbm, hbm, hbm, hbm, hbm],
        out_specs=hbm,
        scratch_shapes=[
            pltpu.VMEM((2, own, depth), bf),
            pltpu.VMEM((SLOTS, depth, wide), bf),
            pltpu.VMEM((CHIPS, kv, tokens, HEAD), bf),
            pltpu.VMEM((CHIPS, kv, HEAD + 16, tokens), bf),
            pltpu.VMEM((kv, own, HEAD), bf),
            pltpu.VMEM((kv, HEAD, own), bf),
            pltpu.VMEM((heads, tokens, HEAD), bf),
            pltpu.VMEM((heads, 1, tokens), f32),
            pltpu.VMEM((heads, HEAD + 16, tokens), f32),
            pltpu.VMEM((own, heads * HEAD), bf),
            pltpu.VMEM((own, heads * HEAD), bf),
            pltpu.VMEM((own, heads * HEAD), bf),
            pltpu.VMEM((own, depth), f32),
            pltpu.VMEM((own, depth), bf),
            pltpu.VMEM((own, own), jnp.int32),
            pltpu.VMEM((tokens, HEAD), f32),
            pltpu.VMEM((tokens, HEAD), f32),
            dma, dma((SLOTS,)), dma, dma, dma, dma((2, 2)), dma((3, 2, 2, 2)), dma((CHIPS, 2, 2, 2)), dma((2, 2)), dma((2, 2)),
            dma((kv,)), dma((kv,)), dma((depth // wide // 2,)),
        ],
        compiler_params=pltpu.CompilerParams(collective_id=0, has_side_effects=True, vmem_limit_bytes=67043328),
        name="layer",
    )(x, gain.reshape(1, depth), wq, wk, wv, wo, table)


def solution(mesh):
    tokens, whole = P(("dp", "sp"), None), P(None, None)
    return jax.shard_map(
        _program,
        mesh=mesh,
        in_specs=(tokens, P(None), whole, whole, whole, whole),
        out_specs=tokens,
        check_vma=False,
    )
```

```python
import functools

import numpy as np
import jax
import jax.numpy as jnp
from jax import lax
from jax.experimental import pallas as pl
from jax.experimental.pallas import tpu as pltpu
from jax.sharding import PartitionSpec as P

HEAD = 128
THETA = 10000
HIDDEN = -2e30
LOG2E = 1.4426950408889634
E2 = HEAD**-0.5 * LOG2E
MESH = pl.DeviceIdType.MESH
CHIPS = 4
SLOTS = 6


def _dot(a, b, ca, cb):
    return lax.dot_general(a, b, (((ca,), (cb,)), ((), ())), preferred_element_type=jnp.float32)


def _tables(rows):
    half = HEAD // 2
    angle = np.arange(rows, dtype=np.float32)[:, None] * np.float32(THETA) ** (-np.arange(half, dtype=np.float32) / np.float32(half))
    angle = angle.astype(np.float32).astype(np.float64)
    return np.concatenate([np.cos(angle), np.sin(angle)], -1).astype(np.float32)


def _score(k, q_ref, h, s_ref, m_ref):
    s = _dot(k, q_ref[h], 1, 1)
    s_ref[...] = s
    m_ref[...] = s.max(axis=0, keepdims=True)


def _take(vt, h, s_ref, m_ref, top_s, mix_s):
    old = top_s[h]
    top = jnp.maximum(old, m_ref[...])
    top_s[h] = top
    p = jnp.exp2((s_ref[...] - top) * E2).astype(jnp.bfloat16)
    mix_s[h] = mix_s[h] * jnp.exp2((old - top) * E2) + _dot(vt, p, 1, 0)


def _score_own(k, q_ref, h, s_ref, m_ref, seen):
    half = seen.shape[0]
    low = jnp.where(seen, _dot(k[:half], q_ref[h, :half], 1, 1), HIDDEN)
    high = _dot(k, q_ref[h, half:], 1, 1)
    above, below = high[:half], jnp.where(seen, high[half:], HIDDEN)
    s_ref[:half, :half] = low
    s_ref[:half, half:] = above
    s_ref[half:, half:] = below
    m_ref[:, :half] = low.max(axis=0, keepdims=True)
    m_ref[:, half:] = jnp.maximum(above, below).max(axis=0, keepdims=True)


def _take_own(vt, h, s_ref, m_ref, top_s, mix_s):
    half = s_ref.shape[0] // 2
    top = m_ref[...]
    top_s[h] = top
    for keys, lanes in ((slice(0, half), slice(0, half)), (slice(None), slice(half, None))):
        p = jnp.exp2((s_ref[keys, lanes] - top[:, lanes]) * E2).astype(jnp.bfloat16)
        mix_s[h, :, lanes] = _dot(vt[:, keys], p, 1, 0)


def _body(x_hbm, gain_ref, wq_hbm, wk_hbm, wv_hbm, wo_hbm, tab_hbm, y_hbm, a_s, w_s, k_s, v_s, km_s, vm_s, q_s, top_s, mix_s, own_s, give_s, got_s,
          acc_s, y_s, s_s, m_s, cos_s, sin_s, x_sem, w_sem, tab_sem, xs_sem, xr_sem, mate_send, send_sem, recv_sem, fsend_sem, frecv_sem,
          swap_send, swap_recv, y_sem):
    own, depth = x_hbm.shape
    tokens = 2 * own
    kv, group = k_s.shape[1], q_s.shape[0] // k_s.shape[1]
    wide = w_s.shape[2]
    per = wide // HEAD
    qcols, kvcols = q_s.shape[0] * HEAD, kv * HEAD
    nq, nkv, pieces = qcols // wide, 4 * kvcols // wide, kv // per
    no = depth // wide
    me = lax.axis_index("sp")
    chip, core = me // 2, me % 2
    mate = chip * 2 + 1 - core
    mine = pl.ds(pl.multiple_of(core * own, own), own)

    plan = [(what, half, p) for p in range(pieces) for half in (1, 0) for what in (0, 1)]

    def kv_block(i):
        what, half, p = plan[i]
        at = pl.multiple_of(lax.rem(core + half, 2) * kvcols + p * wide, wide)
        ref = wk_hbm if what == 0 else wv_hbm
        return pltpu.make_async_copy(ref.at[:, pl.ds(at, wide)], w_s.at[i % SLOTS], w_sem.at[i % SLOTS])

    def q_block(i):
        slot = lax.rem(i + nkv, SLOTS)
        at = pl.multiple_of(core * qcols + i * wide, wide)
        return pltpu.make_async_copy(wq_hbm.at[:, pl.ds(at, wide)], w_s.at[slot], w_sem.at[slot])

    def o_block(i):
        slot = lax.rem(i + nkv + nq, SLOTS)
        rows = pl.multiple_of(jnp.where(i < no, core, 1 - core) * qcols, qcols)
        at = pl.multiple_of(lax.rem(i, no) * wide, wide)
        return pltpu.make_async_copy(wo_hbm.at[pl.ds(rows, qcols), pl.ds(at, wide)], w_s.at[slot, pl.ds(0, qcols), :], w_sem.at[slot])

    load = pltpu.make_async_copy(x_hbm, a_s.at[core], x_sem)
    load.start()
    for i in range(SLOTS):
        kv_block(i).start()
    table = pltpu.make_async_copy(tab_hbm.at[pl.ds(pl.multiple_of(chip * tokens, tokens), tokens)], cos_s, tab_sem)
    table.start()

    barrier = pltpu.get_barrier_semaphore()
    pl.semaphore_signal(barrier, inc=1, device_id={"sp": mate}, device_id_type=MESH)
    for r in (1, 2):
        for g in (0, 1):
            pl.semaphore_signal(barrier, inc=1, device_id={"sp": (chip ^ r) * 2 + g}, device_id_type=MESH)
    pl.semaphore_wait(barrier, 5)

    give = pltpu.make_async_remote_copy(src_ref=x_hbm, dst_ref=a_s.at[core], send_sem=xs_sem, recv_sem=xr_sem, device_id={"sp": mate},
                                        device_id_type=MESH)
    give.start()

    v_s[:, :, HEAD:, :] = jnp.ones((*v_s.shape[:2], v_s.shape[2] - HEAD, v_s.shape[3]), jnp.bfloat16)
    table.wait()
    both = cos_s[...]
    turn = pltpu.roll(both, HEAD // 2, 1)
    left = lax.broadcasted_iota(jnp.int32, both.shape, 1) < HEAD // 2
    cos_s[...] = jnp.where(left, both, turn)
    sin_s[...] = jnp.where(left, -turn, both)

    def turned(t, rows):
        t = t.astype(jnp.float32)
        return (t * cos_s[rows, :] + pltpu.roll(t, HEAD // 2, 1) * sin_s[rows, :]).astype(jnp.bfloat16)

    def normed(slot, keep):
        slab = 16
        gain = gain_ref[...].reshape(1, depth).astype(jnp.float32)

        def one(i, _):
            rows = pl.ds(pl.multiple_of(i * slab, slab), slab)
            t = a_s[slot, rows, :].astype(jnp.float32)
            if keep:
                acc_s[rows, :] = t
            t = t * lax.rsqrt(jnp.mean(t * t, -1, keepdims=True) + 1e-6) * gain
            a_s[slot, rows, :] = t.astype(jnp.bfloat16)
            return 0

        lax.fori_loop(0, own // slab, one, 0, unroll=4)

    def places(what, half, p):
        heads = pl.ds(p * per, per)
        there = k_s.at[chip, heads, mine, :] if what == 0 else v_s.at[chip, heads, pl.ds(0, HEAD), mine]
        if half == 0:
            return there, there
        return (km_s if what == 0 else vm_s).at[heads], there

    def to_mate(what, p):
        src, dst = places(what, 1, p)
        return pltpu.make_async_remote_copy(src_ref=src, dst_ref=dst, send_sem=mate_send.at[what, p], recv_sem=recv_sem.at[chip, core, what, p],
                                            device_id={"sp": mate}, device_id_type=MESH)

    def to_chip(r, what, half, p):
        src, dst = places(what, half, p)
        return pltpu.make_async_remote_copy(src_ref=src, dst_ref=dst, send_sem=send_sem.at[r, what, half, p],
                                            recv_sem=recv_sem.at[chip, core, what, p],
                                            device_id={"sp": (chip ^ r) * 2 + lax.rem(core + half, 2)}, device_id_type=MESH)

    def arrived(there, by, p):
        heads, rows = pl.ds(p * per, per), pl.ds(pl.multiple_of(by * own, own), own)
        for what, ref in ((0, k_s.at[there, heads, rows, :]), (1, v_s.at[there, heads, pl.ds(0, HEAD), rows])):
            pltpu.make_async_remote_copy(src_ref=ref, dst_ref=ref, send_sem=mate_send.at[what, p], recv_sem=recv_sem.at[there, by, what, p],
                                         device_id={"sp": mate}, device_id_type=MESH).wait_recv()

    def passed(source, target, what, p):
        heads = pl.ds(p * per, per)
        ref = k_s.at[source, heads] if what == 0 else v_s.at[source, heads, pl.ds(0, HEAD), :]
        return pltpu.make_async_remote_copy(src_ref=ref, dst_ref=ref, send_sem=fsend_sem.at[what, p], recv_sem=frecv_sem.at[what, p],
                                            device_id={"sp": target * 2 + core}, device_id_type=MESH)

    relay = [(lax.rem(chip, 2) == 1, chip // 2, 3 - chip // 2), (lax.rem(chip, 2) == 0, 1 - chip // 2, 2 + chip // 2)]

    def takes(r, p):
        return ((chip ^ r) > chip) | ((chip == 1) & (r == 1) & (p == 1))

    def given(r, p):
        return ((chip ^ r) < chip) | ((chip == 0) & (r == 1) & (p == 1))

    def from_near(p):
        for r in (1, 2):
            @pl.when(given(r, p))
            def _():
                arrived(chip ^ r, 0, p)
                arrived(chip ^ r, 1, p)
        does, source, target = relay[p]

        @pl.when(does)
        def _():
            for what in (0, 1):
                passed(source, target, what, p).start()

    def send(i):
        for what, half, p in plan[i : i + 2]:
            if half:
                to_mate(what, p).start()
            for r in (1, 2):
                @pl.when(takes(r, p))
                def _():
                    to_chip(r, what, half, p).start()

    load.wait()
    normed(core, True)
    for i in range(0, nkv, 2):
        for m in (i, i + 1):
            kv_block(m).wait()
        if i:
            send(i - 2)
        for m in (i, i + 1):
            what, half, p = plan[m]
            t = _dot(a_s[core], w_s[m % SLOTS], 1, 0)
            for j in range(per):
                u = t[:, j * HEAD : (j + 1) * HEAD]
                n = p * per + j
                if what == 0:
                    u = turned(u.astype(jnp.bfloat16), mine)
                    if half:
                        km_s[n] = u
                    else:
                        k_s[chip, n, mine, :] = u
                else:
                    u = u.T.astype(jnp.bfloat16)
                    if half:
                        vm_s[n] = u
                    else:
                        v_s[chip, n, :HEAD, mine] = u
        for m in (i + SLOTS, i + 1 + SLOTS):
            if m < nkv:
                kv_block(m).start()
            else:
                q_block(m - nkv).start()
    give.wait_recv()
    send(nkv - 2)
    normed(1 - core, False)

    def project(trip, _):
        for j in (0, 1):
            q_block(2 * trip + j).wait()
        for j in (0, 1):
            i = 2 * trip + j
            t = _dot(a_s[...].reshape(tokens, depth), w_s[lax.rem(i + nkv, SLOTS)], 1, 0).astype(jnp.bfloat16)
            for m in range(per):
                q_s[i * per + m] = turned(t[:, m * HEAD : (m + 1) * HEAD], slice(None))
        for j in (0, 1):
            i = 2 * trip + j + SLOTS

            @pl.when(i < nq)
            def _():
                q_block(i).start()

            @pl.when(i >= nq)
            def _():
                o_block(i - nq).start()
        return 0

    lax.fori_loop(0, 3, project, 0)
    from_near(0)
    lax.fori_loop(3, nq // 2, project, 0)

    @pl.when(chip == 0)
    def _():
        from_near(1)

    for p in range(pieces):
        arrived(chip, 1 - core, p)

    part = group // 2
    seen = lax.broadcasted_iota(jnp.int32, (own, own), 1) >= lax.broadcasted_iota(jnp.int32, (own, own), 0)

    def staged(score, take, now, later):
        for j in range(part):
            score(now, part + j, s_s.at[1, j], m_s.at[1, j])
            take(now, j, s_s.at[0, j], m_s.at[0, j])
        for j in range(part):
            score(later, j, s_s.at[0, j], m_s.at[0, j])
            take(now, part + j, s_s.at[1, j], m_s.at[1, j])
        return 0

    def own_score(n, j, s_ref, m_ref):
        _score_own(k_s[chip, n], q_s, n * group + j, s_ref, m_ref, seen)

    def own_take(n, j, s_ref, m_ref):
        _take_own(v_s[chip, n], n * group + j, s_ref, m_ref, top_s, mix_s)

    for j in range(part):
        own_score(0, j, s_s.at[0, j], m_s.at[0, j])
    lax.fori_loop(0, kv, lambda n, _: staged(own_score, own_take, n, jnp.minimum(n + 1, kv - 1)), 0)

    @pl.when(chip > 0)
    def _():
        from_near(1)
        last = chip * kv - 1

        def chunk(t):
            return chip ^ (lax.div(t, kv) + jnp.where(chip == 2, 2, 1)), lax.rem(t, kv)

        def more_score(t, j, s_ref, m_ref):
            there, n = chunk(t)
            _score(k_s[there, n], q_s, n * group + j, s_ref, m_ref)

        def more_take(t, j, s_ref, m_ref):
            there, n = chunk(t)
            _take(v_s[there, n], n * group + j, s_ref, m_ref, top_s, mix_s)

        def more(t, _):
            @pl.when((t + kv == last) & (chip >= 2))
            def _():
                for p in range(pieces):
                    for what in (0, 1):
                        passed(chip ^ 3, chip, what, p).wait_recv()

            return staged(more_score, more_take, t, jnp.minimum(t + 1, last))

        for j in range(part):
            more_score(0, j, s_s.at[0, j], m_s.at[0, j])
        lax.fori_loop(0, last + 1, more, 0)

    def swap(n):
        columns = pl.ds(pl.multiple_of(n * group * HEAD, HEAD), group * HEAD)
        return pltpu.make_async_remote_copy(src_ref=give_s.at[:, columns], dst_ref=got_s.at[:, columns], send_sem=swap_send.at[n],
                                            recv_sem=swap_recv.at[n], device_id={"sp": mate}, device_id_type=MESH)

    def finish(n, _):
        for j in range(group):
            h = n * group + j
            column = pl.ds(pl.multiple_of(h * HEAD, HEAD), HEAD)
            for part, ref in ((core, own_s), (1 - core, give_s)):
                lanes = pl.ds(pl.multiple_of(part * own, own), own)
                t = mix_s[h, :HEAD, lanes] * (1 / mix_s[h, HEAD : HEAD + 1, lanes])
                ref[:, column] = t.T.astype(jnp.bfloat16)

        @pl.when(n > 0)
        def _():
            swap(n - 1).start()
        return 0

    lax.fori_loop(0, kv, finish, 0)

    def out(trip, second):
        for j in (0, 1):
            o_block(2 * trip + j).wait()
        for j in (0, 1):
            i = 2 * trip + j
            column = pl.ds(pl.multiple_of(lax.rem(i, no) * wide, wide), wide)
            t = acc_s[:, column] + _dot((got_s if second else own_s)[...], w_s[lax.rem(i + nkv + nq, SLOTS), :qcols, :], 1, 0)
            if second:
                y_s[:, column] = t.astype(jnp.bfloat16)
            else:
                acc_s[:, column] = t
        for j in (0, 1):
            i = 2 * trip + j + SLOTS

            @pl.when(i < 2 * no)
            def _():
                o_block(i).start()

    def result(i):
        column = pl.ds(pl.multiple_of(i * 2 * wide, wide), 2 * wide)
        return pltpu.make_async_copy(y_s.at[:, column], y_hbm.at[:, column], y_sem.at[i])

    def out_own(trip, _):
        out(trip, False)

        @pl.when(trip == 0)
        def _():
            swap(kv - 1).start()
        return 0

    lax.fori_loop(0, no // 2, out_own, 0)
    for n in range(kv):
        swap(n).wait_recv()

    def out_mate(trip, _):
        out(trip, True)

        @pl.when(trip > no // 2)
        def _():
            result(trip - no // 2 - 1).start()
        return 0

    lax.fori_loop(no // 2, no, out_mate, 0)
    result(no // 2 - 1).start()

    for p in range(pieces):
        for what in (0, 1):
            to_mate(what, p).wait_send()
    for r in (1, 2):
        for p in range(pieces):
            @pl.when(takes(r, p))
            def _():
                for what in (0, 1):
                    for half in (0, 1):
                        to_chip(r, what, half, p).wait_send()
    for p in range(pieces):
        does, source, target = relay[p]

        @pl.when(does)
        def _():
            for what in (0, 1):
                passed(source, target, what, p).wait_send()
    for n in range(kv):
        swap(n).wait_send()
    give.wait_send()
    for i in range(no // 2):
        result(i).wait()


def _program(x, gain, wq, wk, wv, wo):
    own, depth = x.shape
    tokens, heads, kv = 2 * own, wq.shape[1] // HEAD // 2, wk.shape[1] // HEAD // 2
    wide, bf, f32 = 256, jnp.bfloat16, jnp.float32
    table = jnp.asarray(_tables(tokens * CHIPS))
    hbm = pl.BlockSpec(memory_space=pl.ANY)
    dma = pltpu.SemaphoreType.DMA
    return pl.pallas_call(
        _body,
        out_shape=jax.ShapeDtypeStruct((own, depth), bf),
        in_specs=[hbm, pl.BlockSpec(memory_space=pltpu.VMEM), hbm, hbm, hbm, hbm, hbm],
        out_specs=hbm,
        scratch_shapes=[
            pltpu.VMEM((2, own, depth), bf),
            pltpu.VMEM((SLOTS, depth, wide), bf),
            pltpu.VMEM((CHIPS, kv, tokens, HEAD), bf),
            pltpu.VMEM((CHIPS, kv, HEAD + 16, tokens), bf),
            pltpu.VMEM((kv, own, HEAD), bf),
            pltpu.VMEM((kv, HEAD, own), bf),
            pltpu.VMEM((heads, tokens, HEAD), bf),
            pltpu.VMEM((heads, 1, tokens), f32),
            pltpu.VMEM((heads, HEAD + 16, tokens), f32),
            pltpu.VMEM((own, heads * HEAD), bf),
            pltpu.VMEM((own, heads * HEAD), bf),
            pltpu.VMEM((own, heads * HEAD), bf),
            pltpu.VMEM((own, depth), f32),
            pltpu.VMEM((own, depth), bf),
            pltpu.VMEM((2, heads // kv // 2, tokens, tokens), f32),
            pltpu.VMEM((2, heads // kv // 2, 1, tokens), f32),
            pltpu.VMEM((tokens, HEAD), f32),
            pltpu.VMEM((tokens, HEAD), f32),
            dma, dma((SLOTS,)), dma, dma, dma, dma((2, 2)), dma((3, 2, 2, 2)), dma((CHIPS, 2, 2, 2)), dma((2, 2)), dma((2, 2)),
            dma((kv,)), dma((kv,)), dma((depth // wide // 2,)),
        ],
        compiler_params=pltpu.CompilerParams(collective_id=0, has_side_effects=True, vmem_limit_bytes=67043328),
        name="layer",
    )(x, gain, wq, wk, wv, wo, table)


def solution(mesh):
    tokens, whole = P(("dp", "sp"), None), P(None, None)
    return jax.shard_map(
        _program,
        mesh=mesh,
        in_specs=(tokens, P(None), whole, whole, whole, whole),
        out_specs=tokens,
        check_vma=False,
    )
```

```python
import functools

import numpy as np
import jax
import jax.numpy as jnp
from jax import lax
from jax.experimental import pallas as pl
from jax.experimental.pallas import tpu as pltpu
from jax.sharding import PartitionSpec as P

HEAD = 128
THETA = 10000
HIDDEN = -2e30
LOG2E = 1.4426950408889634
E2 = HEAD**-0.5 * LOG2E
MESH = pl.DeviceIdType.MESH
CHIPS = 4
SLOTS = 6


def _dot(a, b, ca, cb):
    return lax.dot_general(a, b, (((ca,), (cb,)), ((), ())), preferred_element_type=jnp.float32)


def _tables(rows):
    half = HEAD // 2
    angle = np.arange(rows, dtype=np.float32)[:, None] * np.float32(THETA) ** (-np.arange(half, dtype=np.float32) / np.float32(half))
    angle = angle.astype(np.float32).astype(np.float64)
    return np.concatenate([np.cos(angle), np.sin(angle)], -1).astype(np.float32)


def _score(k, q_ref, h, s_ref, m_ref):
    s = _dot(k, q_ref[h], 1, 1)
    s_ref[...] = s
    m_ref[...] = s.max(axis=0, keepdims=True)


def _take(vt, h, s_ref, m_ref, top_s, mix_s):
    old = top_s[h]
    top = jnp.maximum(old, m_ref[...])
    top_s[h] = top
    p = jnp.exp2((s_ref[...] - top) * E2).astype(jnp.bfloat16)
    mix_s[h] = mix_s[h] * jnp.exp2((old - top) * E2) + _dot(vt, p, 1, 0)


def _score_own(k, q_ref, h, s_ref, m_ref, seen):
    half = seen.shape[0]
    low = jnp.where(seen, _dot(k[:half], q_ref[h, :half], 1, 1), HIDDEN)
    high = _dot(k, q_ref[h, half:], 1, 1)
    above, below = high[:half], jnp.where(seen, high[half:], HIDDEN)
    s_ref[:half, :half] = low
    s_ref[:half, half:] = above
    s_ref[half:, half:] = below
    m_ref[:, :half] = low.max(axis=0, keepdims=True)
    m_ref[:, half:] = jnp.maximum(above, below).max(axis=0, keepdims=True)


def _take_own(vt, h, s_ref, m_ref, top_s, mix_s):
    half = s_ref.shape[0] // 2
    top = m_ref[...]
    top_s[h] = top
    for keys, lanes in ((slice(0, half), slice(0, half)), (slice(None), slice(half, None))):
        p = jnp.exp2((s_ref[keys, lanes] - top[:, lanes]) * E2).astype(jnp.bfloat16)
        mix_s[h, :, lanes] = _dot(vt[:, keys], p, 1, 0)


def _body(x_hbm, gain_ref, wq_hbm, wk_hbm, wv_hbm, wo_hbm, tab_hbm, y_hbm, a_s, x_s, w_s, k_s, v_s, km_s, vm_s, q_s, top_s, mix_s, own_s, give_s, got_s,
          acc_s, y_s, s_s, m_s, cos_s, sin_s, x_sem, w_sem, tab_sem, xs_sem, xr_sem, mate_send, send_sem, recv_sem, fsend_sem, frecv_sem,
          swap_send, swap_recv, y_sem):
    own, depth = x_hbm.shape
    tokens = 2 * own
    kv, group = k_s.shape[1], q_s.shape[0] // k_s.shape[1]
    wide = w_s.shape[2]
    per = wide // HEAD
    qcols, kvcols = q_s.shape[0] * HEAD, kv * HEAD
    nq, nkv, pieces = qcols // wide, 4 * kvcols // wide, kv // per
    no = depth // wide
    me = lax.axis_index("sp")
    chip, core = me // 2, me % 2
    mate = chip * 2 + 1 - core
    mine = pl.ds(pl.multiple_of(core * own, own), own)

    plan = [(what, half, p) for p in range(pieces) for half in (1, 0) for what in (0, 1)]

    def kv_block(i):
        what, half, p = plan[i]
        at = pl.multiple_of(lax.rem(core + half, 2) * kvcols + p * wide, wide)
        ref = wk_hbm if what == 0 else wv_hbm
        return pltpu.make_async_copy(ref.at[:, pl.ds(at, wide)], w_s.at[i % SLOTS], w_sem.at[i % SLOTS])

    def q_block(i):
        slot = lax.rem(i + nkv, SLOTS)
        at = pl.multiple_of(core * qcols + i * wide, wide)
        return pltpu.make_async_copy(wq_hbm.at[:, pl.ds(at, wide)], w_s.at[slot], w_sem.at[slot])

    def o_block(i):
        slot = lax.rem(i + nkv + nq, SLOTS)
        rows = pl.multiple_of(jnp.where(i < no, core, 1 - core) * qcols, qcols)
        at = pl.multiple_of(lax.rem(i, no) * wide, wide)
        return pltpu.make_async_copy(wo_hbm.at[pl.ds(rows, qcols), pl.ds(at, wide)], w_s.at[slot, pl.ds(0, qcols), :], w_sem.at[slot])

    load = pltpu.make_async_copy(x_hbm, y_s, x_sem)
    load.start()
    table = pltpu.make_async_copy(tab_hbm.at[pl.ds(pl.multiple_of(chip * tokens, tokens), tokens)], cos_s, tab_sem)
    table.start()

    barrier = pltpu.get_barrier_semaphore()
    pl.semaphore_signal(barrier, inc=1, device_id={"sp": mate}, device_id_type=MESH)
    for r in (1, 2):
        for g in (0, 1):
            pl.semaphore_signal(barrier, inc=1, device_id={"sp": (chip ^ r) * 2 + g}, device_id_type=MESH)

    v_s[:, :, HEAD:, :] = jnp.ones((*v_s.shape[:2], v_s.shape[2] - HEAD, v_s.shape[3]), jnp.bfloat16)
    table.wait()
    both = cos_s[...]
    turn = pltpu.roll(both, HEAD // 2, 1)
    left = lax.broadcasted_iota(jnp.int32, both.shape, 1) < HEAD // 2
    cos_s[...] = jnp.where(left, both, turn)
    sin_s[...] = jnp.where(left, -turn, both)

    def turned(t, rows):
        t = t.astype(jnp.float32)
        return (t * cos_s[rows, :] + pltpu.roll(t, HEAD // 2, 1) * sin_s[rows, :]).astype(jnp.bfloat16)

    def normed(ref, slot, keep):
        slab = 16
        gain = gain_ref[...].reshape(1, depth).astype(jnp.float32)

        def one(i, _):
            rows = pl.ds(pl.multiple_of(i * slab, slab), slab)
            t = ref[rows, :].astype(jnp.float32)
            if keep:
                acc_s[rows, :] = t
            t = t * lax.rsqrt(jnp.mean(t * t, -1, keepdims=True) + 1e-6) * gain
            a_s[slot, rows, :] = t.astype(jnp.bfloat16)
            return 0

        lax.fori_loop(0, own // slab, one, 0, unroll=4)

    def places(what, half, p):
        heads = pl.ds(p * per, per)
        there = k_s.at[chip, heads, mine, :] if what == 0 else v_s.at[chip, heads, pl.ds(0, HEAD), mine]
        if half == 0:
            return there, there
        return (km_s if what == 0 else vm_s).at[heads], there

    def to_mate(what, p):
        src, dst = places(what, 1, p)
        return pltpu.make_async_remote_copy(src_ref=src, dst_ref=dst, send_sem=mate_send.at[what, p], recv_sem=recv_sem.at[chip, core, what, p],
                                            device_id={"sp": mate}, device_id_type=MESH)

    def to_chip(r, what, half, p):
        src, dst = places(what, half, p)
        return pltpu.make_async_remote_copy(src_ref=src, dst_ref=dst, send_sem=send_sem.at[r, what, half, p],
                                            recv_sem=recv_sem.at[chip, core, what, p],
                                            device_id={"sp": (chip ^ r) * 2 + lax.rem(core + half, 2)}, device_id_type=MESH)

    def arrived(there, by, p):
        heads, rows = pl.ds(p * per, per), pl.ds(pl.multiple_of(by * own, own), own)
        for what, ref in ((0, k_s.at[there, heads, rows, :]), (1, v_s.at[there, heads, pl.ds(0, HEAD), rows])):
            pltpu.make_async_remote_copy(src_ref=ref, dst_ref=ref, send_sem=mate_send.at[what, p], recv_sem=recv_sem.at[there, by, what, p],
                                         device_id={"sp": mate}, device_id_type=MESH).wait_recv()

    def passed(source, target, what, p):
        heads = pl.ds(p * per, per)
        ref = k_s.at[source, heads] if what == 0 else v_s.at[source, heads, pl.ds(0, HEAD), :]
        return pltpu.make_async_remote_copy(src_ref=ref, dst_ref=ref, send_sem=fsend_sem.at[what, p], recv_sem=frecv_sem.at[what, p],
                                            device_id={"sp": target * 2 + core}, device_id_type=MESH)

    relay = [(lax.rem(chip, 2) == 1, chip // 2, 3 - chip // 2), (lax.rem(chip, 2) == 0, 1 - chip // 2, 2 + chip // 2)]

    def takes(r, p):
        return ((chip ^ r) > chip) | ((chip == 1) & (r == 1) & (p == 1))

    def given(r, p):
        return ((chip ^ r) < chip) | ((chip == 0) & (r == 1) & (p == 1))

    def from_near(p):
        for r in (1, 2):
            @pl.when(given(r, p))
            def _():
                arrived(chip ^ r, 0, p)
                arrived(chip ^ r, 1, p)
        does, source, target = relay[p]

        @pl.when(does)
        def _():
            for what in (0, 1):
                passed(source, target, what, p).start()

    def send(i):
        for what, half, p in plan[i : i + 2]:
            if half:
                to_mate(what, p).start()
            for r in (1, 2):
                @pl.when(takes(r, p))
                def _():
                    to_chip(r, what, half, p).start()

    load.wait()
    for i in range(SLOTS):
        kv_block(i).start()
    normed(y_s, core, True)
    pl.semaphore_wait(barrier, 5)

    give = pltpu.make_async_remote_copy(src_ref=x_hbm, dst_ref=x_s, send_sem=xs_sem, recv_sem=xr_sem, device_id={"sp": mate},
                                        device_id_type=MESH)
    give.start()

    for i in range(0, nkv, 2):
        for m in (i, i + 1):
            kv_block(m).wait()
        if i:
            send(i - 2)
        for m in (i, i + 1):
            what, half, p = plan[m]
            t = _dot(a_s[core], w_s[m % SLOTS], 1, 0)
            for j in range(per):
                u = t[:, j * HEAD : (j + 1) * HEAD]
                n = p * per + j
                if what == 0:
                    u = turned(u.astype(jnp.bfloat16), mine)
                    if half:
                        km_s[n] = u
                    else:
                        k_s[chip, n, mine, :] = u
                else:
                    u = u.T.astype(jnp.bfloat16)
                    if half:
                        vm_s[n] = u
                    else:
                        v_s[chip, n, :HEAD, mine] = u
        for m in (i + SLOTS, i + 1 + SLOTS):
            if m < nkv:
                kv_block(m).start()
            else:
                q_block(m - nkv).start()
    give.wait_recv()
    send(nkv - 2)
    normed(x_s, 1 - core, False)

    def project(trip, _):
        for j in (0, 1):
            q_block(2 * trip + j).wait()
        for j in (0, 1):
            i = 2 * trip + j
            t = _dot(a_s[...].reshape(tokens, depth), w_s[lax.rem(i + nkv, SLOTS)], 1, 0).astype(jnp.bfloat16)
            for m in range(per):
                q_s[i * per + m] = turned(t[:, m * HEAD : (m + 1) * HEAD], slice(None))
        for j in (0, 1):
            i = 2 * trip + j + SLOTS

            @pl.when(i < nq)
            def _():
                q_block(i).start()

            @pl.when(i >= nq)
            def _():
                o_block(i - nq).start()
        return 0

    lax.fori_loop(0, 3, project, 0)
    from_near(0)
    lax.fori_loop(3, nq // 2, project, 0)

    @pl.when(chip == 0)
    def _():
        from_near(1)

    for p in range(pieces):
        arrived(chip, 1 - core, p)

    part = group // 2
    seen = lax.broadcasted_iota(jnp.int32, (own, own), 1) >= lax.broadcasted_iota(jnp.int32, (own, own), 0)

    def staged(score, take, now, later):
        for j in range(part):
            score(now, part + j, s_s.at[1, j], m_s.at[1, j])
            take(now, j, s_s.at[0, j], m_s.at[0, j])
        for j in range(part):
            score(later, j, s_s.at[0, j], m_s.at[0, j])
            take(now, part + j, s_s.at[1, j], m_s.at[1, j])
        return 0

    def own_score(n, j, s_ref, m_ref):
        _score_own(k_s[chip, n], q_s, n * group + j, s_ref, m_ref, seen)

    def own_take(n, j, s_ref, m_ref):
        _take_own(v_s[chip, n], n * group + j, s_ref, m_ref, top_s, mix_s)

    for j in range(part):
        own_score(0, j, s_s.at[0, j], m_s.at[0, j])
    lax.fori_loop(0, kv, lambda n, _: staged(own_score, own_take, n, jnp.minimum(n + 1, kv - 1)), 0)

    @pl.when(chip > 0)
    def _():
        from_near(1)
        last = chip * kv - 1

        def chunk(t):
            return chip ^ (lax.div(t, kv) + jnp.where(chip == 2, 2, 1)), lax.rem(t, kv)

        def more_score(t, j, s_ref, m_ref):
            there, n = chunk(t)
            _score(k_s[there, n], q_s, n * group + j, s_ref, m_ref)

        def more_take(t, j, s_ref, m_ref):
            there, n = chunk(t)
            _take(v_s[there, n], n * group + j, s_ref, m_ref, top_s, mix_s)

        def more(t, _):
            @pl.when((t + kv == last) & (chip >= 2))
            def _():
                for p in range(pieces):
                    for what in (0, 1):
                        passed(chip ^ 3, chip, what, p).wait_recv()

            return staged(more_score, more_take, t, jnp.minimum(t + 1, last))

        for j in range(part):
            more_score(0, j, s_s.at[0, j], m_s.at[0, j])
        lax.fori_loop(0, last + 1, more, 0)

    def swap(n):
        columns = pl.ds(pl.multiple_of(n * group * HEAD, HEAD), group * HEAD)
        return pltpu.make_async_remote_copy(src_ref=give_s.at[:, columns], dst_ref=got_s.at[:, columns], send_sem=swap_send.at[n],
                                            recv_sem=swap_recv.at[n], device_id={"sp": mate}, device_id_type=MESH)

    def finish(n, _):
        for j in range(group):
            h = n * group + j
            column = pl.ds(pl.multiple_of(h * HEAD, HEAD), HEAD)
            for part, ref in ((core, own_s), (1 - core, give_s)):
                lanes = pl.ds(pl.multiple_of(part * own, own), own)
                t = mix_s[h, :HEAD, lanes] * (1 / mix_s[h, HEAD : HEAD + 1, lanes])
                ref[:, column] = t.T.astype(jnp.bfloat16)

        @pl.when(n > 0)
        def _():
            swap(n - 1).start()
        return 0

    lax.fori_loop(0, kv, finish, 0)

    def out(trip, second):
        for j in (0, 1):
            o_block(2 * trip + j).wait()
        for j in (0, 1):
            i = 2 * trip + j
            column = pl.ds(pl.multiple_of(lax.rem(i, no) * wide, wide), wide)
            t = acc_s[:, column] + _dot((got_s if second else own_s)[...], w_s[lax.rem(i + nkv + nq, SLOTS), :qcols, :], 1, 0)
            if second:
                y_s[:, column] = t.astype(jnp.bfloat16)
            else:
                acc_s[:, column] = t
        for j in (0, 1):
            i = 2 * trip + j + SLOTS

            @pl.when(i < 2 * no)
            def _():
                o_block(i).start()

    def result(i):
        column = pl.ds(pl.multiple_of(i * 2 * wide, wide), 2 * wide)
        return pltpu.make_async_copy(y_s.at[:, column], y_hbm.at[:, column], y_sem.at[i])

    def out_own(trip, _):
        out(trip, False)

        @pl.when(trip == 0)
        def _():
            swap(kv - 1).start()
        return 0

    lax.fori_loop(0, no // 2, out_own, 0)
    for n in range(kv):
        swap(n).wait_recv()

    def out_mate(trip, _):
        out(trip, True)

        @pl.when(trip > no // 2)
        def _():
            result(trip - no // 2 - 1).start()
        return 0

    lax.fori_loop(no // 2, no, out_mate, 0)
    result(no // 2 - 1).start()

    for p in range(pieces):
        for what in (0, 1):
            to_mate(what, p).wait_send()
    for r in (1, 2):
        for p in range(pieces):
            @pl.when(takes(r, p))
            def _():
                for what in (0, 1):
                    for half in (0, 1):
                        to_chip(r, what, half, p).wait_send()
    for p in range(pieces):
        does, source, target = relay[p]

        @pl.when(does)
        def _():
            for what in (0, 1):
                passed(source, target, what, p).wait_send()
    for n in range(kv):
        swap(n).wait_send()
    give.wait_send()
    for i in range(no // 2):
        result(i).wait()


def _program(x, gain, wq, wk, wv, wo):
    own, depth = x.shape
    tokens, heads, kv = 2 * own, wq.shape[1] // HEAD // 2, wk.shape[1] // HEAD // 2
    wide, bf, f32 = 256, jnp.bfloat16, jnp.float32
    table = jnp.asarray(_tables(tokens * CHIPS))
    hbm = pl.BlockSpec(memory_space=pl.ANY)
    dma = pltpu.SemaphoreType.DMA
    return pl.pallas_call(
        _body,
        out_shape=jax.ShapeDtypeStruct((own, depth), bf),
        in_specs=[hbm, pl.BlockSpec(memory_space=pltpu.VMEM), hbm, hbm, hbm, hbm, hbm],
        out_specs=hbm,
        scratch_shapes=[
            pltpu.VMEM((2, own, depth), bf),
            pltpu.VMEM((own, depth), bf),
            pltpu.VMEM((SLOTS, depth, wide), bf),
            pltpu.VMEM((CHIPS, kv, tokens, HEAD), bf),
            pltpu.VMEM((CHIPS, kv, HEAD + 16, tokens), bf),
            pltpu.VMEM((kv, own, HEAD), bf),
            pltpu.VMEM((kv, HEAD, own), bf),
            pltpu.VMEM((heads, tokens, HEAD), bf),
            pltpu.VMEM((heads, 1, tokens), f32),
            pltpu.VMEM((heads, HEAD + 16, tokens), f32),
            pltpu.VMEM((own, heads * HEAD), bf),
            pltpu.VMEM((own, heads * HEAD), bf),
            pltpu.VMEM((own, heads * HEAD), bf),
            pltpu.VMEM((own, depth), f32),
            pltpu.VMEM((own, depth), bf),
            pltpu.VMEM((2, heads // kv // 2, tokens, tokens), f32),
            pltpu.VMEM((2, heads // kv // 2, 1, tokens), f32),
            pltpu.VMEM((tokens, HEAD), f32),
            pltpu.VMEM((tokens, HEAD), f32),
            dma, dma((SLOTS,)), dma, dma, dma, dma((2, 2)), dma((3, 2, 2, 2)), dma((CHIPS, 2, 2, 2)), dma((2, 2)), dma((2, 2)),
            dma((kv,)), dma((kv,)), dma((depth // wide // 2,)),
        ],
        compiler_params=pltpu.CompilerParams(collective_id=0, has_side_effects=True, vmem_limit_bytes=67043328),
        name="layer",
    )(x, gain, wq, wk, wv, wo, table)


def solution(mesh):
    tokens, whole = P(("dp", "sp"), None), P(None, None)
    return jax.shard_map(
        _program,
        mesh=mesh,
        in_specs=(tokens, P(None), whole, whole, whole, whole),
        out_specs=tokens,
        check_vma=False,
    )
```

```python
import functools

import numpy as np
import jax
import jax.numpy as jnp
from jax import lax
from jax.experimental import pallas as pl
from jax.experimental.pallas import tpu as pltpu
from jax.sharding import PartitionSpec as P

HEAD = 128
THETA = 10000
HIDDEN = -2e30
LOG2E = 1.4426950408889634
E2 = HEAD**-0.5 * LOG2E
MESH = pl.DeviceIdType.MESH
CHIPS = 4
SLOTS = 6


def _dot(a, b, ca, cb):
    return lax.dot_general(a, b, (((ca,), (cb,)), ((), ())), preferred_element_type=jnp.float32)


def _tables(rows):
    half = HEAD // 2
    angle = np.arange(rows, dtype=np.float32)[:, None] * np.float32(THETA) ** (-np.arange(half, dtype=np.float32) / np.float32(half))
    angle = angle.astype(np.float32).astype(np.float64)
    return np.concatenate([np.cos(angle), np.sin(angle)], -1).astype(np.float32)


def _score(k, q_ref, h, s_ref, m_ref):
    s = _dot(k, q_ref[h], 1, 1)
    s_ref[...] = s
    m_ref[...] = s.max(axis=0, keepdims=True)


def _take(vt, h, s_ref, m_ref, top_s, mix_s):
    old = top_s[h]
    top = jnp.maximum(old, m_ref[...])
    top_s[h] = top
    p = jnp.exp2((s_ref[...] - top) * E2).astype(jnp.bfloat16)
    mix_s[h] = mix_s[h] * jnp.exp2((old - top) * E2) + _dot(vt, p, 1, 0)


def _score_own(k, q_ref, h, s_ref, m_ref, seen):
    half = seen.shape[0]
    low = jnp.where(seen, _dot(k[:half], q_ref[h, :half], 1, 1), HIDDEN)
    high = _dot(k, q_ref[h, half:], 1, 1)
    above, below = high[:half], jnp.where(seen, high[half:], HIDDEN)
    s_ref[:half, :half] = low
    s_ref[:half, half:] = above
    s_ref[half:, half:] = below
    m_ref[:, :half] = low.max(axis=0, keepdims=True)
    m_ref[:, half:] = jnp.maximum(above, below).max(axis=0, keepdims=True)


def _take_own(vt, h, s_ref, m_ref, top_s, mix_s):
    half = s_ref.shape[0] // 2
    top = m_ref[...]
    top_s[h] = top
    for keys, lanes in ((slice(0, half), slice(0, half)), (slice(None), slice(half, None))):
        p = jnp.exp2((s_ref[keys, lanes] - top[:, lanes]) * E2).astype(jnp.bfloat16)
        mix_s[h, :, lanes] = _dot(vt[:, keys], p, 1, 0)


def _body(x_hbm, gain_ref, wq_hbm, wk_hbm, wv_hbm, wo_hbm, tab_hbm, y_hbm, a_s, x_s, w_s, k_s, v_s, km_s, vm_s, q_s, top_s, mix_s, own_s, give_s, got_s,
          extra_s, acc_s, y_s, s_s, m_s, cos_s, sin_s, x_sem, w_sem, tab_sem, xs_sem, xr_sem, mate_send, send_sem, recv_sem, fsend_sem, frecv_sem,
          swap_send, swap_recv, q_send, q_recv, back_send, back_recv, late_sem, y_sem):
    own, depth = x_hbm.shape
    tokens = 2 * own
    kv, qcols = k_s.shape[1], own_s.shape[1]
    group = qcols // HEAD // kv
    late = group * HEAD
    wide = w_s.shape[2]
    per = wide // HEAD
    kvcols = kv * HEAD
    nq, nkv, pieces = qcols // wide, 4 * kvcols // wide, kv // per
    no = depth // wide
    me = lax.axis_index("sp")
    chip, core = me // 2, me % 2
    mate = chip * 2 + 1 - core
    mine = pl.ds(pl.multiple_of(core * own, own), own)

    plan = [(what, half, p) for p in range(pieces) for half in (1, 0) for what in (0, 1)]

    def kv_block(i):
        what, half, p = plan[i]
        at = pl.multiple_of(lax.rem(core + half, 2) * kvcols + p * wide, wide)
        ref = wk_hbm if what == 0 else wv_hbm
        return pltpu.make_async_copy(ref.at[:, pl.ds(at, wide)], w_s.at[i % SLOTS], w_sem.at[i % SLOTS])

    def q_place(i):
        return lax.rem(i + nq - group // per, nq)

    def q_block(i):
        slot = lax.rem(i + nkv, SLOTS)
        at = pl.multiple_of(core * qcols + q_place(i) * wide, wide)
        return pltpu.make_async_copy(wq_hbm.at[:, pl.ds(at, wide)], w_s.at[slot], w_sem.at[slot])

    def o_part(i, half, first, count, to, sem):
        slot = lax.rem(i + nkv + nq, SLOTS)
        rows = pl.multiple_of(lax.rem(core + half, 2) * qcols + first, HEAD)
        at = pl.multiple_of(lax.rem(i, no) * wide, wide)
        return pltpu.make_async_copy(wo_hbm.at[pl.ds(rows, count), pl.ds(at, wide)], w_s.at[slot, pl.ds(to, count), :], sem.at[slot])

    def o_block(i, do):
        @pl.when(i < 2 * no)
        def _():
            do(o_part(i, lax.div(i, no), 0, qcols - late, 0, w_sem))

        @pl.when(i >= 2 * no)
        def _():
            do(o_part(i, 0, qcols - late, late, 0, w_sem))
            do(o_part(i, 1, qcols - late, late, late, late_sem))

    load = pltpu.make_async_copy(x_hbm, y_s, x_sem)
    load.start()
    table = pltpu.make_async_copy(tab_hbm.at[pl.ds(pl.multiple_of(chip * tokens, tokens), tokens)], cos_s, tab_sem)
    table.start()

    barrier = pltpu.get_barrier_semaphore()
    pl.semaphore_signal(barrier, inc=1, device_id={"sp": mate}, device_id_type=MESH)
    for r in (1, 2, 3):
        for g in (0, 1):
            pl.semaphore_signal(barrier, inc=1, device_id={"sp": (chip ^ r) * 2 + g}, device_id_type=MESH)

    v_s[:, :, HEAD:, :] = jnp.ones((*v_s.shape[:2], v_s.shape[2] - HEAD, v_s.shape[3]), jnp.bfloat16)
    table.wait()
    both = cos_s[...]
    turn = pltpu.roll(both, HEAD // 2, 1)
    left = lax.broadcasted_iota(jnp.int32, both.shape, 1) < HEAD // 2
    cos_s[...] = jnp.where(left, both, turn)
    sin_s[...] = jnp.where(left, -turn, both)

    def turned(t, rows):
        t = t.astype(jnp.float32)
        return (t * cos_s[rows, :] + pltpu.roll(t, HEAD // 2, 1) * sin_s[rows, :]).astype(jnp.bfloat16)

    def normed(ref, slot, keep):
        slab = 16
        gain = gain_ref[...].reshape(1, depth).astype(jnp.float32)

        def one(i, _):
            rows = pl.ds(pl.multiple_of(i * slab, slab), slab)
            t = ref[rows, :].astype(jnp.float32)
            if keep:
                acc_s[rows, :] = t
            t = t * lax.rsqrt(jnp.mean(t * t, -1, keepdims=True) + 1e-6) * gain
            a_s[slot, rows, :] = t.astype(jnp.bfloat16)
            return 0

        lax.fori_loop(0, own // slab, one, 0, unroll=4)

    def places(what, half, p):
        heads = pl.ds(p * per, per)
        there = k_s.at[chip, heads, mine, :] if what == 0 else v_s.at[chip, heads, pl.ds(0, HEAD), mine]
        if half == 0:
            return there, there
        return (km_s if what == 0 else vm_s).at[heads], there

    def to_mate(what, p):
        src, dst = places(what, 1, p)
        return pltpu.make_async_remote_copy(src_ref=src, dst_ref=dst, send_sem=mate_send.at[what, p], recv_sem=recv_sem.at[chip, core, what, p],
                                            device_id={"sp": mate}, device_id_type=MESH)

    def to_chip(r, what, half, p):
        src, dst = places(what, half, p)
        return pltpu.make_async_remote_copy(src_ref=src, dst_ref=dst, send_sem=send_sem.at[r, what, half, p],
                                            recv_sem=recv_sem.at[chip, core, what, p],
                                            device_id={"sp": (chip ^ r) * 2 + lax.rem(core + half, 2)}, device_id_type=MESH)

    def arrived(there, by, p):
        heads, rows = pl.ds(p * per, per), pl.ds(pl.multiple_of(by * own, own), own)
        for what, ref in ((0, k_s.at[there, heads, rows, :]), (1, v_s.at[there, heads, pl.ds(0, HEAD), rows])):
            pltpu.make_async_remote_copy(src_ref=ref, dst_ref=ref, send_sem=mate_send.at[what, p], recv_sem=recv_sem.at[there, by, what, p],
                                         device_id={"sp": mate}, device_id_type=MESH).wait_recv()

    def passed(source, target, what, p):
        heads = pl.ds(p * per, per)
        ref = k_s.at[source, heads] if what == 0 else v_s.at[source, heads, pl.ds(0, HEAD), :]
        return pltpu.make_async_remote_copy(src_ref=ref, dst_ref=ref, send_sem=fsend_sem.at[what, p], recv_sem=frecv_sem.at[what, p],
                                            device_id={"sp": target * 2 + core}, device_id_type=MESH)

    relay = [(lax.rem(chip, 2) == 1, chip // 2, 3 - chip // 2), (lax.rem(chip, 2) == 0, 1 - chip // 2, 2 + chip // 2)]

    def takes(r, p):
        later = (chip ^ r) > chip if r < 3 else False
        return later | ((chip == r) & (p == 1))

    def given(r, p):
        return ((chip ^ r) < chip) | ((chip == 0) & (r == 1) & (p == 1))

    def from_near(p):
        for r in (1, 2):
            @pl.when(given(r, p))
            def _():
                arrived(chip ^ r, 0, p)
                arrived(chip ^ r, 1, p)
        does, source, target = relay[p]

        @pl.when(does)
        def _():
            for what in (0, 1):
                passed(source, target, what, p).start()

    def send(i):
        for what, half, p in plan[i : i + 2]:
            if half:
                to_mate(what, p).start()
            for r in (1, 2, 3)[: 2 + p]:
                @pl.when(takes(r, p))
                def _():
                    to_chip(r, what, half, p).start()

    load.wait()
    for i in range(SLOTS):
        kv_block(i).start()
    normed(y_s, core, True)
    pl.semaphore_wait(barrier, 7)

    give = pltpu.make_async_remote_copy(src_ref=x_hbm, dst_ref=x_s, send_sem=xs_sem, recv_sem=xr_sem, device_id={"sp": mate},
                                        device_id_type=MESH)
    give.start()

    for i in range(0, nkv, 2):
        for m in (i, i + 1):
            kv_block(m).wait()
        if i:
            send(i - 2)
        for m in (i, i + 1):
            what, half, p = plan[m]
            t = _dot(a_s[core], w_s[m % SLOTS], 1, 0)
            for j in range(per):
                u = t[:, j * HEAD : (j + 1) * HEAD]
                n = p * per + j
                if what == 0:
                    u = turned(u.astype(jnp.bfloat16), mine)
                    if half:
                        km_s[n] = u
                    else:
                        k_s[chip, n, mine, :] = u
                else:
                    u = u.T.astype(jnp.bfloat16)
                    if half:
                        vm_s[n] = u
                    else:
                        v_s[chip, n, :HEAD, mine] = u
        for m in (i + SLOTS, i + 1 + SLOTS):
            if m < nkv:
                kv_block(m).start()
            else:
                q_block(m - nkv).start()
    give.wait_recv()
    send(nkv - 2)
    normed(x_s, 1 - core, False)

    def lent(i):
        at, count = (0, 2 * per) if i == 0 else (2 * per, group - 2 * per)
        return pltpu.make_async_remote_copy(src_ref=q_s.at[pl.ds((kv - 1) * group + at, count)], dst_ref=q_s.at[pl.ds(kv * group + at, count)],
                                            send_sem=q_send.at[i], recv_sem=q_recv.at[i], device_id={"sp": (chip ^ 3) * 2 + core},
                                            device_id_type=MESH)

    def project(trip, _):
        for j in (0, 1):
            q_block(2 * trip + j).wait()
        for i in (0, 1):
            @pl.when((chip == 3) & (trip == i + 1))
            def _():
                lent(i).start()

        @pl.when(trip == 3)
        def _():
            from_near(0)

        for j in (0, 1):
            i = 2 * trip + j
            t = _dot(a_s[...].reshape(tokens, depth), w_s[lax.rem(i + nkv, SLOTS)], 1, 0).astype(jnp.bfloat16)
            for m in range(per):
                q_s[q_place(i) * per + m] = turned(t[:, m * HEAD : (m + 1) * HEAD], slice(None))
        for j in (0, 1):
            i = 2 * trip + j + SLOTS

            @pl.when(i < nq)
            def _():
                q_block(i).start()

            @pl.when(i >= nq)
            def _():
                o_block(i - nq, lambda c: c.start())
        return 0

    lax.fori_loop(0, nq // 2, project, 0)

    @pl.when(chip == 0)
    def _():
        from_near(1)

    for p in range(pieces):
        arrived(chip, 1 - core, p)

    part = group // 2
    seen = lax.broadcasted_iota(jnp.int32, (own, own), 1) >= lax.broadcasted_iota(jnp.int32, (own, own), 0)

    def staged(score, take, now, later):
        for j in range(part):
            score(now, part + j, s_s.at[1, j], m_s.at[1, j])
            take(now, j, s_s.at[0, j], m_s.at[0, j])
        for j in range(part):
            score(later, j, s_s.at[0, j], m_s.at[0, j])
            take(now, part + j, s_s.at[1, j], m_s.at[1, j])
        return 0

    owns = kv + jnp.where(chip == 0, 1, 0) - jnp.where(chip == 3, 1, 0)

    def own_place(n):
        return jnp.where(n == kv, 3, chip), jnp.minimum(n, kv - 1)

    def own_score(n, j, s_ref, m_ref):
        there, head = own_place(n)
        _score_own(k_s[there, head], q_s, n * group + j, s_ref, m_ref, seen)

    def own_take(n, j, s_ref, m_ref):
        there, head = own_place(n)
        _take_own(v_s[there, head], n * group + j, s_ref, m_ref, top_s, mix_s)

    def owned(n, _):
        @pl.when((chip == 0) & (n == kv - 1))
        def _():
            for i in (0, 1):
                lent(i).wait_recv()
            for there in (2, 3):
                arrived(there, 0, 1)
                arrived(there, 1, 1)

        return staged(own_score, own_take, n, jnp.minimum(n + 1, owns - 1))

    for j in range(part):
        own_score(0, j, s_s.at[0, j], m_s.at[0, j])
    lax.fori_loop(0, owns, owned, 0)

    @pl.when(chip > 0)
    def _():
        from_near(1)

    heads = jnp.where(chip == 0, 1, jnp.where(chip == 3, kv - 1, kv))
    last = jnp.where(chip == 0, 3, chip) * heads - 1

    def chunk(t):
        i = lax.div(t, heads)
        n = lax.rem(t, heads)
        return (jnp.where(chip == 0, i, chip ^ (i + jnp.where(chip == 2, 2, 1))), jnp.where(chip == 0, kv - 1, n), jnp.where(chip == 0, kv, n))

    def more_score(t, j, s_ref, m_ref):
        there, head, n = chunk(t)
        _score(k_s[there, head], q_s, n * group + j, s_ref, m_ref)

    def more_take(t, j, s_ref, m_ref):
        there, head, n = chunk(t)
        _take(v_s[there, head], n * group + j, s_ref, m_ref, top_s, mix_s)

    def more(t, _):
        @pl.when((t + heads == last) & (chip >= 2))
        def _():
            for p in range(pieces):
                for what in (0, 1):
                    passed(chip ^ 3, chip, what, p).wait_recv()

        return staged(more_score, more_take, t, jnp.minimum(t + 1, last))

    for j in range(part):
        more_score(0, j, s_s.at[0, j], m_s.at[0, j])
    lax.fori_loop(0, last + 1, more, 0)

    def swap(n):
        columns = pl.ds(pl.multiple_of(n * group * HEAD, HEAD), group * HEAD)
        return pltpu.make_async_remote_copy(src_ref=give_s.at[:, columns], dst_ref=got_s.at[:, columns], send_sem=swap_send.at[n],
                                            recv_sem=swap_recv.at[n], device_id={"sp": mate}, device_id_type=MESH)

    def settled(n, own_ref, give_ref, at):
        for j in range(group):
            h = n * group + j
            column = pl.ds(pl.multiple_of(at + j * HEAD, HEAD), HEAD)
            for part, ref in ((core, own_ref), (1 - core, give_ref)):
                lanes = pl.ds(pl.multiple_of(part * own, own), own)
                t = mix_s[h, :HEAD, lanes] * (1 / mix_s[h, HEAD : HEAD + 1, lanes])
                ref[:, column] = t.T.astype(jnp.bfloat16)

    def back(i):
        return pltpu.make_async_remote_copy(src_ref=extra_s.at[i], dst_ref=(own_s, got_s)[i].at[:, pl.ds(qcols - late, late)],
                                            send_sem=back_send.at[i], recv_sem=back_recv.at[i],
                                            device_id={"sp": (chip ^ 3) * 2 + (core if i == 0 else 1 - core)}, device_id_type=MESH)

    @pl.when(chip == 0)
    def _():
        settled(kv, extra_s.at[0], extra_s.at[1], 0)

    swaps = jnp.where(chip == 3, kv - 1, kv)

    def finish(n, _):
        settled(n, own_s, give_s, n * late)

        @pl.when((chip == 0) & (n == 0))
        def _():
            for i in (0, 1):
                back(i).start()

        @pl.when(n > 0)
        def _():
            swap(n - 1).start()
        return 0

    lax.fori_loop(0, swaps, finish, 0)

    def out(trip, phase):
        for j in (0, 1):
            o_block(2 * trip + j, lambda c: c.wait())
        for j in (0, 1):
            i = 2 * trip + j
            column = pl.ds(pl.multiple_of(lax.rem(i, no) * wide, wide), wide)
            w = w_s.at[lax.rem(i + nkv + nq, SLOTS)]
            if phase < 2:
                t = _dot((own_s, got_s)[phase][:, : qcols - late], w[: qcols - late, :], 1, 0)
            else:
                t = _dot(own_s[:, qcols - late :], w[:late, :], 1, 0) + _dot(got_s[:, qcols - late :], w[late : 2 * late, :], 1, 0)
            t = acc_s[:, column] + t
            if phase == 2:
                y_s[:, column] = t.astype(jnp.bfloat16)
            else:
                acc_s[:, column] = t
        for j in (0, 1):
            i = 2 * trip + j + SLOTS

            @pl.when(i < 3 * no)
            def _():
                o_block(i, lambda c: c.start())

    def result(i):
        column = pl.ds(pl.multiple_of(i * 2 * wide, wide), 2 * wide)
        return pltpu.make_async_copy(y_s.at[:, column], y_hbm.at[:, column], y_sem.at[i])

    trips = no // 2

    def out_own(trip, _):
        out(trip, 0)

        @pl.when(trip == 0)
        def _():
            swap(swaps - 1).start()
        return 0

    def out_mate(trip, _):
        out(trip, 1)
        return 0

    def out_late(trip, _):
        out(trip, 2)

        @pl.when(trip > 2 * trips)
        def _():
            result(trip - 2 * trips - 1).start()
        return 0

    lax.fori_loop(0, trips, out_own, 0)
    for n in range(kv - 1):
        swap(n).wait_recv()
    lax.fori_loop(trips, 2 * trips, out_mate, 0)

    @pl.when(chip == 3)
    def _():
        for i in (0, 1):
            back(i).wait_recv()

    @pl.when(chip < 3)
    def _():
        swap(kv - 1).wait_recv()

    lax.fori_loop(2 * trips, 3 * trips, out_late, 0)
    result(trips - 1).start()

    for p in range(pieces):
        for what in (0, 1):
            to_mate(what, p).wait_send()
    for r in (1, 2, 3):
        for p in range(r // 3, pieces):
            @pl.when(takes(r, p))
            def _():
                for what in (0, 1):
                    for half in (0, 1):
                        to_chip(r, what, half, p).wait_send()
    for p in range(pieces):
        does, source, target = relay[p]

        @pl.when(does)
        def _():
            for what in (0, 1):
                passed(source, target, what, p).wait_send()
    for n in range(kv - 1):
        swap(n).wait_send()

    @pl.when(chip < 3)
    def _():
        swap(kv - 1).wait_send()

    for i in (0, 1):
        @pl.when(chip == 3)
        def _():
            lent(i).wait_send()

        @pl.when(chip == 0)
        def _():
            back(i).wait_send()

    give.wait_send()
    for i in range(no // 2):
        result(i).wait()


def _program(x, gain, wq, wk, wv, wo):
    own, depth = x.shape
    tokens, heads, kv = 2 * own, wq.shape[1] // HEAD // 2, wk.shape[1] // HEAD // 2
    group, wide, bf, f32 = heads // kv, 256, jnp.bfloat16, jnp.float32
    table = jnp.asarray(_tables(tokens * CHIPS))
    hbm = pl.BlockSpec(memory_space=pl.ANY)
    dma = pltpu.SemaphoreType.DMA
    return pl.pallas_call(
        _body,
        out_shape=jax.ShapeDtypeStruct((own, depth), bf),
        in_specs=[hbm, pl.BlockSpec(memory_space=pltpu.VMEM), hbm, hbm, hbm, hbm, hbm],
        out_specs=hbm,
        scratch_shapes=[
            pltpu.VMEM((2, own, depth), bf),
            pltpu.VMEM((own, depth), bf),
            pltpu.VMEM((SLOTS, depth, wide), bf),
            pltpu.VMEM((CHIPS, kv, tokens, HEAD), bf),
            pltpu.VMEM((CHIPS, kv, HEAD + 16, tokens), bf),
            pltpu.VMEM((kv, own, HEAD), bf),
            pltpu.VMEM((kv, HEAD, own), bf),
            pltpu.VMEM((heads + group, tokens, HEAD), bf),
            pltpu.VMEM((heads + group, 1, tokens), f32),
            pltpu.VMEM((heads + group, HEAD + 16, tokens), f32),
            pltpu.VMEM((own, heads * HEAD), bf),
            pltpu.VMEM((own, heads * HEAD), bf),
            pltpu.VMEM((own, heads * HEAD), bf),
            pltpu.VMEM((2, own, group * HEAD), bf),
            pltpu.VMEM((own, depth), f32),
            pltpu.VMEM((own, depth), bf),
            pltpu.VMEM((2, heads // kv // 2, tokens, tokens), f32),
            pltpu.VMEM((2, heads // kv // 2, 1, tokens), f32),
            pltpu.VMEM((tokens, HEAD), f32),
            pltpu.VMEM((tokens, HEAD), f32),
            dma, dma((SLOTS,)), dma, dma, dma, dma((2, 2)), dma((4, 2, 2, 2)), dma((CHIPS, 2, 2, 2)), dma((2, 2)), dma((2, 2)),
            dma((kv,)), dma((kv,)), dma((2,)), dma((2,)), dma((2,)), dma((2,)), dma((SLOTS,)), dma((depth // wide // 2,)),
        ],
        compiler_params=pltpu.CompilerParams(collective_id=0, has_side_effects=True, vmem_limit_bytes=67043328),
        name="layer",
    )(x, gain, wq, wk, wv, wo, table)


def solution(mesh):
    tokens, whole = P(("dp", "sp"), None), P(None, None)
    return jax.shard_map(
        _program,
        mesh=mesh,
        in_specs=(tokens, P(None), whole, whole, whole, whole),
        out_specs=tokens,
        check_vma=False,
    )
```

```python
import functools

import numpy as np
import jax
import jax.numpy as jnp
from jax import lax
from jax.experimental import pallas as pl
from jax.experimental.pallas import tpu as pltpu
from jax.sharding import PartitionSpec as P

HEAD = 128
THETA = 10000
HIDDEN = -2e30
LOG2E = 1.4426950408889634
E2 = HEAD**-0.5 * LOG2E
MESH = pl.DeviceIdType.MESH
CHIPS = 4
SLOTS = 6


def _dot(a, b, ca, cb):
    return lax.dot_general(a, b, (((ca,), (cb,)), ((), ())), preferred_element_type=jnp.float32)


def _tables(rows):
    half = HEAD // 2
    angle = np.arange(rows, dtype=np.float32)[:, None] * np.float32(THETA) ** (-np.arange(half, dtype=np.float32) / np.float32(half))
    angle = angle.astype(np.float32).astype(np.float64)
    return np.concatenate([np.cos(angle), np.sin(angle)], -1).astype(np.float32)


def _score(k, q_ref, h, s_ref, m_ref):
    s = _dot(k, q_ref[h], 1, 1)
    s_ref[...] = s
    m_ref[...] = s.max(axis=0, keepdims=True)


def _take(vt, h, s_ref, m_ref, top_s, mix_s):
    old = top_s[h]
    top = jnp.maximum(old, m_ref[...])
    top_s[h] = top
    p = jnp.exp2((s_ref[...] - top) * E2).astype(jnp.bfloat16)
    mix_s[h] = mix_s[h] * jnp.exp2((old - top) * E2) + _dot(vt, p, 1, 0)


def _score_own(k, q_ref, h, s_ref, m_ref, seen):
    half = seen.shape[0]
    low = jnp.where(seen, _dot(k[:half], q_ref[h, :half], 1, 1), HIDDEN)
    high = _dot(k, q_ref[h, half:], 1, 1)
    above, below = high[:half], jnp.where(seen, high[half:], HIDDEN)
    s_ref[:half, :half] = low
    s_ref[:half, half:] = above
    s_ref[half:, half:] = below
    m_ref[:, :half] = low.max(axis=0, keepdims=True)
    m_ref[:, half:] = jnp.maximum(above, below).max(axis=0, keepdims=True)


def _take_own(vt, h, s_ref, m_ref, top_s, mix_s):
    half = s_ref.shape[0] // 2
    top = m_ref[...]
    top_s[h] = top
    for keys, lanes in ((slice(0, half), slice(0, half)), (slice(None), slice(half, None))):
        p = jnp.exp2((s_ref[keys, lanes] - top[:, lanes]) * E2).astype(jnp.bfloat16)
        mix_s[h, :, lanes] = _dot(vt[:, keys], p, 1, 0)


def _body(x_hbm, gain_ref, wq_hbm, wk_hbm, wv_hbm, wo_hbm, tab_hbm, y_hbm, a_s, x_s, w_s, k_s, v_s, km_s, vm_s, q_s, top_s, mix_s, own_s, give_s, got_s,
          acc_s, y_s, s_s, m_s, cos_s, sin_s, x_sem, w_sem, tab_sem, xs_sem, xr_sem, mate_send, send_sem, recv_sem, fsend_sem, frecv_sem,
          swap_send, swap_recv, y_sem):
    own, depth = x_hbm.shape
    tokens = 2 * own
    kv, group = k_s.shape[1], q_s.shape[0] // k_s.shape[1]
    wide = w_s.shape[2]
    per = wide // HEAD
    qcols, kvcols = q_s.shape[0] * HEAD, kv * HEAD
    nq, nkv, pieces = qcols // wide, 4 * kvcols // wide, kv // per
    no = depth // wide
    me = lax.axis_index("sp")
    chip, core = me // 2, me % 2
    mate = chip * 2 + 1 - core
    mine = pl.ds(pl.multiple_of(core * own, own), own)

    plan = [(what, half, p) for p in range(pieces) for half in (1, 0) for what in (0, 1)]

    def kv_block(i):
        what, half, p = plan[i]
        at = pl.multiple_of(lax.rem(core + half, 2) * kvcols + p * wide, wide)
        ref = wk_hbm if what == 0 else wv_hbm
        return pltpu.make_async_copy(ref.at[:, pl.ds(at, wide)], w_s.at[i % SLOTS], w_sem.at[i % SLOTS])

    def q_block(i):
        slot = lax.rem(i + nkv, SLOTS)
        at = pl.multiple_of(core * qcols + i * wide, wide)
        return pltpu.make_async_copy(wq_hbm.at[:, pl.ds(at, wide)], w_s.at[slot], w_sem.at[slot])

    def o_block(i):
        slot = lax.rem(i + nkv + nq, SLOTS)
        rows = pl.multiple_of(jnp.where(i < no, core, 1 - core) * qcols, qcols)
        at = pl.multiple_of(lax.rem(i, no) * wide, wide)
        return pltpu.make_async_copy(wo_hbm.at[pl.ds(rows, qcols), pl.ds(at, wide)], w_s.at[slot, pl.ds(0, qcols), :], w_sem.at[slot])

    load = pltpu.make_async_copy(x_hbm, y_s, x_sem)
    load.start()
    table = pltpu.make_async_copy(tab_hbm.at[pl.ds(pl.multiple_of(chip * tokens, tokens), tokens)], cos_s, tab_sem)
    table.start()

    barrier = pltpu.get_barrier_semaphore()
    pl.semaphore_signal(barrier, inc=1, device_id={"sp": mate}, device_id_type=MESH)
    for r in (1, 2):
        for g in (0, 1):
            pl.semaphore_signal(barrier, inc=1, device_id={"sp": (chip ^ r) * 2 + g}, device_id_type=MESH)

    v_s[:, :, HEAD:, :] = jnp.ones((*v_s.shape[:2], v_s.shape[2] - HEAD, v_s.shape[3]), jnp.bfloat16)
    table.wait()
    both = cos_s[...]
    turn = pltpu.roll(both, HEAD // 2, 1)
    left = lax.broadcasted_iota(jnp.int32, both.shape, 1) < HEAD // 2
    cos_s[...] = jnp.where(left, both, turn)
    sin_s[...] = jnp.where(left, -turn, both)

    def turned(t, rows):
        t = t.astype(jnp.float32)
        return (t * cos_s[rows, :] + pltpu.roll(t, HEAD // 2, 1) * sin_s[rows, :]).astype(jnp.bfloat16)

    def normed(ref, slot, keep):
        slab = 16
        gain = gain_ref[...].reshape(1, depth).astype(jnp.float32)

        def one(i, _):
            rows = pl.ds(pl.multiple_of(i * slab, slab), slab)
            t = ref[rows, :].astype(jnp.float32)
            if keep:
                acc_s[rows, :] = t
            t = t * lax.rsqrt(jnp.mean(t * t, -1, keepdims=True) + 1e-6) * gain
            a_s[slot, rows, :] = t.astype(jnp.bfloat16)
            return 0

        lax.fori_loop(0, own // slab, one, 0, unroll=4 if keep else True)

    def places(what, half, p):
        heads = pl.ds(p * per, per)
        there = k_s.at[chip, heads, mine, :] if what == 0 else v_s.at[chip, heads, pl.ds(0, HEAD), mine]
        if half == 0:
            return there, there
        return (km_s if what == 0 else vm_s).at[heads], there

    def to_mate(what, p):
        src, dst = places(what, 1, p)
        return pltpu.make_async_remote_copy(src_ref=src, dst_ref=dst, send_sem=mate_send.at[what, p], recv_sem=recv_sem.at[chip, core, what, p],
                                            device_id={"sp": mate}, device_id_type=MESH)

    def to_chip(r, what, half, p):
        src, dst = places(what, half, p)
        return pltpu.make_async_remote_copy(src_ref=src, dst_ref=dst, send_sem=send_sem.at[r, what, half, p],
                                            recv_sem=recv_sem.at[chip, core, what, p],
                                            device_id={"sp": (chip ^ r) * 2 + lax.rem(core + half, 2)}, device_id_type=MESH)

    def arrived(there, by, what, p):
        heads, rows = pl.ds(p * per, per), pl.ds(pl.multiple_of(by * own, own), own)
        ref = k_s.at[there, heads, rows, :] if what == 0 else v_s.at[there, heads, pl.ds(0, HEAD), rows]
        pltpu.make_async_remote_copy(src_ref=ref, dst_ref=ref, send_sem=mate_send.at[what, p], recv_sem=recv_sem.at[there, by, what, p],
                                     device_id={"sp": mate}, device_id_type=MESH).wait_recv()

    def passed(source, target, what, p):
        heads = pl.ds(p * per, per)
        ref = k_s.at[source, heads] if what == 0 else v_s.at[source, heads, pl.ds(0, HEAD), :]
        return pltpu.make_async_remote_copy(src_ref=ref, dst_ref=ref, send_sem=fsend_sem.at[what, p], recv_sem=frecv_sem.at[what, p],
                                            device_id={"sp": target * 2 + core}, device_id_type=MESH)

    source = jnp.where((chip == 0) | (chip == 3), 1, 0)

    def takes(r, what):
        later = (chip ^ r) > chip
        return later | (chip == r) if (r, what) == (1, 0) else later

    def from_near(p):
        for r in (1, 2):
            for what in (0, 1):
                near = (chip ^ r) < chip

                @pl.when(near | (chip == 0) if (r, what) == (1, 0) else near)
                def _():
                    arrived(chip ^ r, 0, what, p)
                    arrived(chip ^ r, 1, what, p)
        for what in (0, 1):
            @pl.when(chip // 2 == what)
            def _():
                passed(source, 3 - source, what, p).start()

    def send(i):
        for what, half, p in plan[i : i + 2]:
            if half:
                to_mate(what, p).start()
            for r in (1, 2):
                @pl.when(takes(r, what))
                def _():
                    to_chip(r, what, half, p).start()

    load.wait()
    for i in range(SLOTS):
        kv_block(i).start()
    normed(y_s, core, True)
    pl.semaphore_wait(barrier, 5)

    give = pltpu.make_async_remote_copy(src_ref=x_hbm, dst_ref=x_s, send_sem=xs_sem, recv_sem=xr_sem, device_id={"sp": mate},
                                        device_id_type=MESH)
    give.start()

    for i in range(0, nkv, 2):
        for m in (i, i + 1):
            kv_block(m).wait()
        if i:
            send(i - 2)
        if i == nkv - 2:
            give.wait_recv()
            normed(x_s, 1 - core, False)
        for m in (i, i + 1):
            what, half, p = plan[m]
            t = _dot(a_s[core], w_s[m % SLOTS], 1, 0)
            for j in range(per):
                u = t[:, j * HEAD : (j + 1) * HEAD]
                n = p * per + j
                if what == 0:
                    u = turned(u.astype(jnp.bfloat16), mine)
                    if half:
                        km_s[n] = u
                    else:
                        k_s[chip, n, mine, :] = u
                else:
                    u = u.T.astype(jnp.bfloat16)
                    if half:
                        vm_s[n] = u
                    else:
                        v_s[chip, n, :HEAD, mine] = u
        for m in (i + SLOTS, i + 1 + SLOTS):
            if m < nkv:
                kv_block(m).start()
            else:
                q_block(m - nkv).start()
    send(nkv - 2)

    def project(trip, _):
        for j in range(3):
            q_block(3 * trip + j).wait()
        for j in range(3):
            i = 3 * trip + j
            t = _dot(a_s[...].reshape(tokens, depth), w_s[lax.rem(i + nkv, SLOTS)], 1, 0).astype(jnp.bfloat16)
            for m in range(per):
                q_s[i * per + m] = turned(t[:, m * HEAD : (m + 1) * HEAD], slice(None))
        for j in range(3):
            i = 3 * trip + j + SLOTS

            @pl.when(i < nq)
            def _():
                q_block(i).start()

            @pl.when(i >= nq)
            def _():
                o_block(i - nq).start()
        return 0

    lax.fori_loop(0, 2, project, 0)
    from_near(0)
    lax.fori_loop(2, nq // 3, project, 0)

    for p in range(pieces):
        for what in (0, 1):
            arrived(chip, 1 - core, what, p)

    part = group // 2
    seen = lax.broadcasted_iota(jnp.int32, (own, own), 1) >= lax.broadcasted_iota(jnp.int32, (own, own), 0)

    def staged(score, take, now, later):
        for j in range(part):
            score(now, part + j, s_s.at[1, j], m_s.at[1, j])
            take(now, j, s_s.at[0, j], m_s.at[0, j])
        for j in range(part):
            score(later, j, s_s.at[0, j], m_s.at[0, j])
            take(now, part + j, s_s.at[1, j], m_s.at[1, j])
        return 0

    def own_score(n, j, s_ref, m_ref):
        _score_own(k_s[chip, n], q_s, n * group + j, s_ref, m_ref, seen)

    def own_take(n, j, s_ref, m_ref):
        _take_own(v_s[chip, n], n * group + j, s_ref, m_ref, top_s, mix_s)

    for j in range(part):
        own_score(0, j, s_s.at[0, j], m_s.at[0, j])
    lax.fori_loop(0, kv, lambda n, _: staged(own_score, own_take, n, jnp.minimum(n + 1, kv - 1)), 0)

    @pl.when(chip < 3)
    def _():
        from_near(1)

    @pl.when(chip > 0)
    def _():
        last = chip * kv - 1

        def chunk(t):
            return chip ^ (lax.div(t, kv) + jnp.where(chip == 2, 2, 1)), lax.rem(t, kv)

        def more_score(t, j, s_ref, m_ref):
            there, n = chunk(t)
            _score(k_s[there, n], q_s, n * group + j, s_ref, m_ref)

        def more_take(t, j, s_ref, m_ref):
            there, n = chunk(t)
            _take(v_s[there, n], n * group + j, s_ref, m_ref, top_s, mix_s)

        def more(t, _):
            @pl.when((chip == 3) & (t == 1))
            def _():
                from_near(1)

            for p in range(pieces):
                @pl.when((t + kv == last + p * per) & (chip >= 2))
                def _():
                    for what in (0, 1):
                        passed(chip ^ 3, chip, what, p).wait_recv()

            return staged(more_score, more_take, t, jnp.minimum(t + 1, last))

        for j in range(part):
            more_score(0, j, s_s.at[0, j], m_s.at[0, j])
        lax.fori_loop(0, last + 1, more, 0)

    def swap(n):
        columns = pl.ds(pl.multiple_of(n * group * HEAD, HEAD), group * HEAD)
        return pltpu.make_async_remote_copy(src_ref=give_s.at[:, columns], dst_ref=got_s.at[:, columns], send_sem=swap_send.at[n],
                                            recv_sem=swap_recv.at[n], device_id={"sp": mate}, device_id_type=MESH)

    def finish(n, _):
        for j in range(group):
            h = n * group + j
            column = pl.ds(pl.multiple_of(h * HEAD, HEAD), HEAD)
            for part, ref in ((core, own_s), (1 - core, give_s)):
                lanes = pl.ds(pl.multiple_of(part * own, own), own)
                t = mix_s[h, :HEAD, lanes] * (1 / mix_s[h, HEAD : HEAD + 1, lanes])
                ref[:, column] = t.T.astype(jnp.bfloat16)

        @pl.when(n > 0)
        def _():
            swap(n - 1).start()
        return 0

    lax.fori_loop(0, kv, finish, 0)

    def out(trip, second):
        for j in (0, 1):
            o_block(2 * trip + j).wait()
        for j in (0, 1):
            i = 2 * trip + j
            column = pl.ds(pl.multiple_of(lax.rem(i, no) * wide, wide), wide)
            t = acc_s[:, column] + _dot((got_s if second else own_s)[...], w_s[lax.rem(i + nkv + nq, SLOTS), :qcols, :], 1, 0)
            if second:
                y_s[:, column] = t.astype(jnp.bfloat16)
            else:
                acc_s[:, column] = t
        for j in (0, 1):
            i = 2 * trip + j + SLOTS

            @pl.when(i < 2 * no)
            def _():
                o_block(i).start()

    def result(i):
        column = pl.ds(pl.multiple_of(i * 2 * wide, wide), 2 * wide)
        return pltpu.make_async_copy(y_s.at[:, column], y_hbm.at[:, column], y_sem.at[i])

    def out_own(trip, _):
        out(trip, False)

        @pl.when(trip == 0)
        def _():
            swap(kv - 1).start()
        return 0

    lax.fori_loop(0, no // 2, out_own, 0)
    for n in range(kv):
        swap(n).wait_recv()

    def out_mate(trip, _):
        out(trip, True)

        @pl.when(trip > no // 2)
        def _():
            result(trip - no // 2 - 1).start()
        return 0

    lax.fori_loop(no // 2, no, out_mate, 0)
    result(no // 2 - 1).start()

    for p in range(pieces):
        for what in (0, 1):
            to_mate(what, p).wait_send()
    for r in (1, 2):
        for what in (0, 1):
            @pl.when(takes(r, what))
            def _():
                for p in range(pieces):
                    for half in (0, 1):
                        to_chip(r, what, half, p).wait_send()
    for what in (0, 1):
        @pl.when(chip // 2 == what)
        def _():
            for p in range(pieces):
                passed(source, 3 - source, what, p).wait_send()
    for n in range(kv):
        swap(n).wait_send()
    give.wait_send()
    for i in range(no // 2):
        result(i).wait()


def _program(x, gain, wq, wk, wv, wo):
    own, depth = x.shape
    tokens, heads, kv = 2 * own, wq.shape[1] // HEAD // 2, wk.shape[1] // HEAD // 2
    wide, bf, f32 = 256, jnp.bfloat16, jnp.float32
    table = jnp.asarray(_tables(tokens * CHIPS))
    hbm = pl.BlockSpec(memory_space=pl.ANY)
    dma = pltpu.SemaphoreType.DMA
    return pl.pallas_call(
        _body,
        out_shape=jax.ShapeDtypeStruct((own, depth), bf),
        in_specs=[hbm, pl.BlockSpec(memory_space=pltpu.VMEM), hbm, hbm, hbm, hbm, hbm],
        out_specs=hbm,
        scratch_shapes=[
            pltpu.VMEM((2, own, depth), bf),
            pltpu.VMEM((own, depth), bf),
            pltpu.VMEM((SLOTS, depth, wide), bf),
            pltpu.VMEM((CHIPS, kv, tokens, HEAD), bf),
            pltpu.VMEM((CHIPS, kv, HEAD + 16, tokens), bf),
            pltpu.VMEM((kv, own, HEAD), bf),
            pltpu.VMEM((kv, HEAD, own), bf),
            pltpu.VMEM((heads, tokens, HEAD), bf),
            pltpu.VMEM((heads, 1, tokens), f32),
            pltpu.VMEM((heads, HEAD + 16, tokens), f32),
            pltpu.VMEM((own, heads * HEAD), bf),
            pltpu.VMEM((own, heads * HEAD), bf),
            pltpu.VMEM((own, heads * HEAD), bf),
            pltpu.VMEM((own, depth), f32),
            pltpu.VMEM((own, depth), bf),
            pltpu.VMEM((2, heads // kv // 2, tokens, tokens), f32),
            pltpu.VMEM((2, heads // kv // 2, 1, tokens), f32),
            pltpu.VMEM((tokens, HEAD), f32),
            pltpu.VMEM((tokens, HEAD), f32),
            dma, dma((SLOTS,)), dma, dma, dma, dma((2, 2)), dma((3, 2, 2, 2)), dma((CHIPS, 2, 2, 2)), dma((2, 2)), dma((2, 2)),
            dma((kv,)), dma((kv,)), dma((depth // wide // 2,)),
        ],
        compiler_params=pltpu.CompilerParams(collective_id=0, has_side_effects=True, vmem_limit_bytes=67043328),
        name="layer",
    )(x, gain, wq, wk, wv, wo, table)


def solution(mesh):
    tokens, whole = P(("dp", "sp"), None), P(None, None)
    return jax.shard_map(
        _program,
        mesh=mesh,
        in_specs=(tokens, P(None), whole, whole, whole, whole),
        out_specs=tokens,
        check_vma=False,
    )
```

```python
import functools

import numpy as np
import jax
import jax.numpy as jnp
from jax import lax
from jax.experimental import pallas as pl
from jax.experimental.pallas import tpu as pltpu
from jax.sharding import PartitionSpec as P

HEAD = 128
THETA = 10000
HIDDEN = -2e30
LOG2E = 1.4426950408889634
E2 = HEAD**-0.5 * LOG2E
MESH = pl.DeviceIdType.MESH
CHIPS = 4
SLOTS = 6


def _dot(a, b, ca, cb):
    return lax.dot_general(a, b, (((ca,), (cb,)), ((), ())), preferred_element_type=jnp.float32)


def _tables(rows):
    half = HEAD // 2
    angle = np.arange(rows, dtype=np.float32)[:, None] * np.float32(THETA) ** (-np.arange(half, dtype=np.float32) / np.float32(half))
    angle = angle.astype(np.float32).astype(np.float64)
    return np.concatenate([np.cos(angle), np.sin(angle)], -1).astype(np.float32)


def _score(k, q_ref, h, s_ref, m_ref):
    s = _dot(k, q_ref[h], 1, 1)
    s_ref[...] = s
    m_ref[...] = s.max(axis=0, keepdims=True)


def _take(vt, h, s_ref, m_ref, top_s, mix_s):
    old = top_s[h]
    top = jnp.maximum(old, m_ref[...])
    top_s[h] = top
    p = jnp.exp2((s_ref[...] - top) * E2).astype(jnp.bfloat16)
    mix_s[h] = mix_s[h] * jnp.exp2((old - top) * E2) + _dot(vt, p, 1, 0)


def _score_own(k, q_ref, h, s_ref, m_ref, seen):
    half = seen.shape[0]
    low = jnp.where(seen, _dot(k[:half], q_ref[h, :half], 1, 1), HIDDEN)
    high = _dot(k, q_ref[h, half:], 1, 1)
    above, below = high[:half], jnp.where(seen, high[half:], HIDDEN)
    s_ref[:half, :half] = low
    s_ref[:half, half:] = above
    s_ref[half:, half:] = below
    m_ref[:, :half] = low.max(axis=0, keepdims=True)
    m_ref[:, half:] = jnp.maximum(above, below).max(axis=0, keepdims=True)


def _take_own(vt, h, s_ref, m_ref, top_s, mix_s):
    half = s_ref.shape[0] // 2
    top = m_ref[...]
    top_s[h] = top
    for keys, lanes in ((slice(0, half), slice(0, half)), (slice(None), slice(half, None))):
        p = jnp.exp2((s_ref[keys, lanes] - top[:, lanes]) * E2).astype(jnp.bfloat16)
        mix_s[h, :, lanes] = _dot(vt[:, keys], p, 1, 0)


def _body(x_hbm, gain_ref, wq_hbm, wk_hbm, wv_hbm, wo_hbm, tab_hbm, y_hbm, a_s, x_s, w_s, k_s, v_s, km_s, vm_s, q_s, top_s, mix_s, own_s, give_s, got_s,
          acc_s, y_s, s_s, m_s, cos_s, sin_s, x_sem, w_sem, tab_sem, xs_sem, xr_sem, mate_send, send_sem, recv_sem, fsend_sem, frecv_sem,
          swap_send, swap_recv, y_sem):
    own, depth = x_hbm.shape
    tokens = 2 * own
    kv, group = k_s.shape[1], q_s.shape[0] // k_s.shape[1]
    wide = w_s.shape[2]
    per = wide // HEAD
    qcols, kvcols = q_s.shape[0] * HEAD, kv * HEAD
    nq, nkv, pieces = qcols // wide, 4 * kvcols // wide, kv // per
    no = depth // wide
    me = lax.axis_index("sp")
    chip, core = me // 2, me % 2
    mate = chip * 2 + 1 - core
    mine = pl.ds(pl.multiple_of(core * own, own), own)

    plan = [(what, half, p) for p in range(pieces) for half in (1, 0) for what in (0, 1)]

    def kv_block(i):
        what, half, p = plan[i]
        at = pl.multiple_of(lax.rem(core + half, 2) * kvcols + p * wide, wide)
        ref = wk_hbm if what == 0 else wv_hbm
        return pltpu.make_async_copy(ref.at[:, pl.ds(at, wide)], w_s.at[i % SLOTS], w_sem.at[i % SLOTS])

    def q_block(i):
        slot = lax.rem(i + nkv, SLOTS)
        at = pl.multiple_of(core * qcols + i * wide, wide)
        return pltpu.make_async_copy(wq_hbm.at[:, pl.ds(at, wide)], w_s.at[slot], w_sem.at[slot])

    def o_block(i):
        slot = lax.rem(i + nkv + nq, SLOTS)
        rows = pl.multiple_of(jnp.where(i < no, core, 1 - core) * qcols, qcols)
        at = pl.multiple_of(lax.rem(i, no) * wide, wide)
        return pltpu.make_async_copy(wo_hbm.at[pl.ds(rows, qcols), pl.ds(at, wide)], w_s.at[slot, pl.ds(0, qcols), :], w_sem.at[slot])

    load = pltpu.make_async_copy(x_hbm, y_s, x_sem)
    load.start()
    table = pltpu.make_async_copy(tab_hbm.at[pl.ds(pl.multiple_of(chip * tokens, tokens), tokens)], cos_s, tab_sem)
    table.start()

    barrier = pltpu.get_barrier_semaphore()
    pl.semaphore_signal(barrier, inc=1, device_id={"sp": mate}, device_id_type=MESH)
    for r in (1, 2):
        for g in (0, 1):
            pl.semaphore_signal(barrier, inc=1, device_id={"sp": (chip ^ r) * 2 + g}, device_id_type=MESH)

    v_s[:, :, HEAD:, :] = jnp.ones((*v_s.shape[:2], v_s.shape[2] - HEAD, v_s.shape[3]), jnp.bfloat16)
    table.wait()
    both = cos_s[...]
    turn = pltpu.roll(both, HEAD // 2, 1)
    left = lax.broadcasted_iota(jnp.int32, both.shape, 1) < HEAD // 2
    cos_s[...] = jnp.where(left, both, turn)
    sin_s[...] = jnp.where(left, -turn, both)

    def turned(t, rows):
        t = t.astype(jnp.float32)
        return (t * cos_s[rows, :] + pltpu.roll(t, HEAD // 2, 1) * sin_s[rows, :]).astype(jnp.bfloat16)

    def normed(ref, slot, keep):
        slab = 16
        gain = gain_ref[...].reshape(1, depth).astype(jnp.float32)

        def one(i, _):
            rows = pl.ds(pl.multiple_of(i * slab, slab), slab)
            t = ref[rows, :].astype(jnp.float32)
            if keep:
                acc_s[rows, :] = t
            t = t * lax.rsqrt(jnp.mean(t * t, -1, keepdims=True) + 1e-6) * gain
            a_s[slot, rows, :] = t.astype(jnp.bfloat16)
            return 0

        lax.fori_loop(0, own // slab, one, 0, unroll=4 if keep else True)

    def places(what, half, p):
        heads = pl.ds(p * per, per)
        there = k_s.at[chip, heads, mine, :] if what == 0 else v_s.at[chip, heads, pl.ds(0, HEAD), mine]
        if half == 0:
            return there, there
        return (km_s if what == 0 else vm_s).at[heads], there

    def to_mate(what, p):
        src, dst = places(what, 1, p)
        return pltpu.make_async_remote_copy(src_ref=src, dst_ref=dst, send_sem=mate_send.at[what, p], recv_sem=recv_sem.at[chip, core, what, p],
                                            device_id={"sp": mate}, device_id_type=MESH)

    def to_chip(r, what, half, p):
        src, dst = places(what, half, p)
        return pltpu.make_async_remote_copy(src_ref=src, dst_ref=dst, send_sem=send_sem.at[r, what, half, p],
                                            recv_sem=recv_sem.at[chip, core, what, p],
                                            device_id={"sp": (chip ^ r) * 2 + lax.rem(core + half, 2)}, device_id_type=MESH)

    def arrived(there, by, what, p):
        heads, rows = pl.ds(p * per, per), pl.ds(pl.multiple_of(by * own, own), own)
        ref = k_s.at[there, heads, rows, :] if what == 0 else v_s.at[there, heads, pl.ds(0, HEAD), rows]
        pltpu.make_async_remote_copy(src_ref=ref, dst_ref=ref, send_sem=mate_send.at[what, p], recv_sem=recv_sem.at[there, by, what, p],
                                     device_id={"sp": mate}, device_id_type=MESH).wait_recv()

    def passed(source, target, what, p):
        heads = pl.ds(p * per, per)
        ref = k_s.at[source, heads] if what == 0 else v_s.at[source, heads, pl.ds(0, HEAD), :]
        return pltpu.make_async_remote_copy(src_ref=ref, dst_ref=ref, send_sem=fsend_sem.at[what, p], recv_sem=frecv_sem.at[what, p],
                                            device_id={"sp": target * 2 + core}, device_id_type=MESH)

    source = jnp.where((chip == 0) | (chip == 3), 1, 0)

    def takes(r, what):
        later = (chip ^ r) > chip
        return later | (chip == r) if (r, what) == (1, 0) else later

    def from_near(p):
        for r in (1, 2):
            for what in (0, 1):
                near = (chip ^ r) < chip

                @pl.when(near | (chip == 0) if (r, what) == (1, 0) else near)
                def _():
                    arrived(chip ^ r, 0, what, p)
                    arrived(chip ^ r, 1, what, p)
        for what in (0, 1):
            @pl.when(chip // 2 == what)
            def _():
                passed(source, 3 - source, what, p).start()

    def send(i):
        for what, half, p in plan[i : i + 2]:
            if half:
                to_mate(what, p).start()
            for r in (1, 2):
                @pl.when(takes(r, what))
                def _():
                    to_chip(r, what, half, p).start()

    load.wait()
    for i in range(SLOTS):
        kv_block(i).start()
    normed(y_s, core, True)
    pl.semaphore_wait(barrier, 5)

    give = pltpu.make_async_remote_copy(src_ref=x_hbm, dst_ref=x_s, send_sem=xs_sem, recv_sem=xr_sem, device_id={"sp": mate},
                                        device_id_type=MESH)
    give.start()

    for i in range(0, nkv, 2):
        for m in (i, i + 1):
            kv_block(m).wait()
        if i:
            send(i - 2)
        if i == nkv - 2:
            give.wait_recv()
            normed(x_s, 1 - core, False)
        for m in (i, i + 1):
            what, half, p = plan[m]
            t = _dot(a_s[core], w_s[m % SLOTS], 1, 0)
            for j in range(per):
                u = t[:, j * HEAD : (j + 1) * HEAD]
                n = p * per + j
                if what == 0:
                    u = turned(u.astype(jnp.bfloat16), mine)
                    if half:
                        km_s[n] = u
                    else:
                        k_s[chip, n, mine, :] = u
                else:
                    u = u.T.astype(jnp.bfloat16)
                    if half:
                        vm_s[n] = u
                    else:
                        v_s[chip, n, :HEAD, mine] = u
        for m in (i + SLOTS, i + 1 + SLOTS):
            if m < nkv:
                kv_block(m).start()
            else:
                q_block(m - nkv).start()
    send(nkv - 2)

    def project(trip, _):
        for j in range(3):
            q_block(3 * trip + j).wait()
        for j in range(3):
            i = 3 * trip + j
            t = _dot(a_s[...].reshape(tokens, depth), w_s[lax.rem(i + nkv, SLOTS)], 1, 0).astype(jnp.bfloat16)
            for m in range(per):
                q_s[i * per + m] = turned(t[:, m * HEAD : (m + 1) * HEAD], slice(None))
        for j in range(3):
            i = 3 * trip + j + SLOTS

            @pl.when(i < nq)
            def _():
                q_block(i).start()

            @pl.when(i >= nq)
            def _():
                o_block(i - nq).start()
        return 0

    lax.fori_loop(0, 2, project, 0)
    from_near(0)
    lax.fori_loop(2, nq // 3, project, 0)

    for p in range(pieces):
        for what in (0, 1):
            arrived(chip, 1 - core, what, p)

    part = group // 2
    seen = lax.broadcasted_iota(jnp.int32, (own, own), 1) >= lax.broadcasted_iota(jnp.int32, (own, own), 0)

    def staged(score, take, now, later):
        order = [(now, 0), (now, part), (now + 1, 0), (now + 1, part), (later, 0)]
        for i in range(4):
            (n, at), (ahead, to) = order[i], order[i + 1]
            for j in range(part):
                score(ahead, to + j, s_s.at[(i + 1) % 2, j], m_s.at[(i + 1) % 2, j])
                take(n, at + j, s_s.at[i % 2, j], m_s.at[i % 2, j])
        return 0

    def own_score(n, j, s_ref, m_ref):
        _score_own(k_s[chip, n], q_s, n * group + j, s_ref, m_ref, seen)

    def own_take(n, j, s_ref, m_ref):
        _take_own(v_s[chip, n], n * group + j, s_ref, m_ref, top_s, mix_s)

    for j in range(part):
        own_score(0, j, s_s.at[0, j], m_s.at[0, j])
    lax.fori_loop(0, kv // 2, lambda i, _: staged(own_score, own_take, 2 * i, jnp.minimum(2 * i + 2, kv - 1)), 0)

    @pl.when(chip < 3)
    def _():
        from_near(1)

    @pl.when(chip > 0)
    def _():
        last = chip * kv - 1

        def chunk(t):
            return chip ^ (lax.div(t, kv) + jnp.where(chip == 2, 2, 1)), lax.rem(t, kv)

        def more_score(t, j, s_ref, m_ref):
            there, n = chunk(t)
            _score(k_s[there, n], q_s, n * group + j, s_ref, m_ref)

        def more_take(t, j, s_ref, m_ref):
            there, n = chunk(t)
            _take(v_s[there, n], n * group + j, s_ref, m_ref, top_s, mix_s)

        def more(i, _):
            t = 2 * i
            @pl.when((chip == 3) & (t == 0))
            def _():
                from_near(1)

            for p in range(pieces):
                @pl.when((t + 1 + kv == last + p * per) & (chip >= 2))
                def _():
                    for what in (0, 1):
                        passed(chip ^ 3, chip, what, p).wait_recv()

            return staged(more_score, more_take, t, jnp.minimum(t + 2, last))

        for j in range(part):
            more_score(0, j, s_s.at[0, j], m_s.at[0, j])
        lax.fori_loop(0, (last + 1) // 2, more, 0)

    def swap(n):
        columns = pl.ds(pl.multiple_of(n * group * HEAD, HEAD), group * HEAD)
        return pltpu.make_async_remote_copy(src_ref=give_s.at[:, columns], dst_ref=got_s.at[:, columns], send_sem=swap_send.at[n],
                                            recv_sem=swap_recv.at[n], device_id={"sp": mate}, device_id_type=MESH)

    def finish(n, _):
        for j in range(group):
            h = n * group + j
            column = pl.ds(pl.multiple_of(h * HEAD, HEAD), HEAD)
            for part, ref in ((core, own_s), (1 - core, give_s)):
                lanes = pl.ds(pl.multiple_of(part * own, own), own)
                t = mix_s[h, :HEAD, lanes] * (1 / mix_s[h, HEAD : HEAD + 1, lanes])
                ref[:, column] = t.T.astype(jnp.bfloat16)

        @pl.when(n > 0)
        def _():
            swap(n - 1).start()
        return 0

    lax.fori_loop(0, kv, finish, 0)

    def out(trip, second):
        for j in (0, 1):
            o_block(2 * trip + j).wait()
        for j in (0, 1):
            i = 2 * trip + j
            column = pl.ds(pl.multiple_of(lax.rem(i, no) * wide, wide), wide)
            t = acc_s[:, column] + _dot((got_s if second else own_s)[...], w_s[lax.rem(i + nkv + nq, SLOTS), :qcols, :], 1, 0)
            if second:
                y_s[:, column] = t.astype(jnp.bfloat16)
            else:
                acc_s[:, column] = t
        for j in (0, 1):
            i = 2 * trip + j + SLOTS

            @pl.when(i < 2 * no)
            def _():
                o_block(i).start()

    def result(i):
        column = pl.ds(pl.multiple_of(i * 2 * wide, wide), 2 * wide)
        return pltpu.make_async_copy(y_s.at[:, column], y_hbm.at[:, column], y_sem.at[i])

    def out_own(trip, _):
        out(trip, False)

        @pl.when(trip == 0)
        def _():
            swap(kv - 1).start()
        return 0

    lax.fori_loop(0, no // 2, out_own, 0)
    for n in range(kv):
        swap(n).wait_recv()

    def out_mate(trip, _):
        out(trip, True)

        @pl.when(trip > no // 2)
        def _():
            result(trip - no // 2 - 1).start()
        return 0

    lax.fori_loop(no // 2, no, out_mate, 0)
    result(no // 2 - 1).start()

    for p in range(pieces):
        for what in (0, 1):
            to_mate(what, p).wait_send()
    for r in (1, 2):
        for what in (0, 1):
            @pl.when(takes(r, what))
            def _():
                for p in range(pieces):
                    for half in (0, 1):
                        to_chip(r, what, half, p).wait_send()
    for what in (0, 1):
        @pl.when(chip // 2 == what)
        def _():
            for p in range(pieces):
                passed(source, 3 - source, what, p).wait_send()
    for n in range(kv):
        swap(n).wait_send()
    give.wait_send()
    for i in range(no // 2):
        result(i).wait()


def _program(x, gain, wq, wk, wv, wo):
    own, depth = x.shape
    tokens, heads, kv = 2 * own, wq.shape[1] // HEAD // 2, wk.shape[1] // HEAD // 2
    wide, bf, f32 = 256, jnp.bfloat16, jnp.float32
    table = jnp.asarray(_tables(tokens * CHIPS))
    hbm = pl.BlockSpec(memory_space=pl.ANY)
    dma = pltpu.SemaphoreType.DMA
    return pl.pallas_call(
        _body,
        out_shape=jax.ShapeDtypeStruct((own, depth), bf),
        in_specs=[hbm, pl.BlockSpec(memory_space=pltpu.VMEM), hbm, hbm, hbm, hbm, hbm],
        out_specs=hbm,
        scratch_shapes=[
            pltpu.VMEM((2, own, depth), bf),
            pltpu.VMEM((own, depth), bf),
            pltpu.VMEM((SLOTS, depth, wide), bf),
            pltpu.VMEM((CHIPS, kv, tokens, HEAD), bf),
            pltpu.VMEM((CHIPS, kv, HEAD + 16, tokens), bf),
            pltpu.VMEM((kv, own, HEAD), bf),
            pltpu.VMEM((kv, HEAD, own), bf),
            pltpu.VMEM((heads, tokens, HEAD), bf),
            pltpu.VMEM((heads, 1, tokens), f32),
            pltpu.VMEM((heads, HEAD + 16, tokens), f32),
            pltpu.VMEM((own, heads * HEAD), bf),
            pltpu.VMEM((own, heads * HEAD), bf),
            pltpu.VMEM((own, heads * HEAD), bf),
            pltpu.VMEM((own, depth), f32),
            pltpu.VMEM((own, depth), bf),
            pltpu.VMEM((2, heads // kv // 2, tokens, tokens), f32),
            pltpu.VMEM((2, heads // kv // 2, 1, tokens), f32),
            pltpu.VMEM((tokens, HEAD), f32),
            pltpu.VMEM((tokens, HEAD), f32),
            dma, dma((SLOTS,)), dma, dma, dma, dma((2, 2)), dma((3, 2, 2, 2)), dma((CHIPS, 2, 2, 2)), dma((2, 2)), dma((2, 2)),
            dma((kv,)), dma((kv,)), dma((depth // wide // 2,)),
        ],
        compiler_params=pltpu.CompilerParams(collective_id=0, has_side_effects=True, vmem_limit_bytes=67043328),
        name="layer",
    )(x, gain, wq, wk, wv, wo, table)


def _copy_body(x_hbm, y_hbm, buf, in_sem, out_sem):
    parts, rows = buf.shape[:2]

    def take(i):
        return pltpu.make_async_copy(x_hbm.at[pl.ds(i * rows, rows)], buf.at[i], in_sem.at[i])

    def put(i):
        return pltpu.make_async_copy(buf.at[i], y_hbm.at[pl.ds(i * rows, rows)], out_sem.at[i])

    for i in range(parts):
        take(i).start()
    for i in range(parts):
        take(i).wait()
        put(i).start()
    for i in range(parts):
        put(i).wait()


def _copied(x, parts=8):
    hbm, dma = pl.BlockSpec(memory_space=pl.ANY), pltpu.SemaphoreType.DMA
    return pl.pallas_call(
        _copy_body,
        out_shape=jax.ShapeDtypeStruct(x.shape, x.dtype),
        in_specs=[hbm],
        out_specs=hbm,
        scratch_shapes=[pltpu.VMEM((parts, x.shape[0] // parts, x.shape[1]), x.dtype), dma((parts,)), dma((parts,))],
        compiler_params=pltpu.CompilerParams(vmem_limit_bytes=67043328),
        name="copied",
    )(x)


def solution(mesh):
    tokens, whole = P(("dp", "sp"), None), P(None, None)
    return jax.shard_map(
        lambda *args: _copied(_program(*args)),
        mesh=mesh,
        in_specs=(tokens, P(None), whole, whole, whole, whole),
        out_specs=tokens,
        check_vma=False,
    )
```

```python
import functools

import numpy as np
import jax
import jax.numpy as jnp
from jax import lax
from jax.experimental import pallas as pl
from jax.experimental.pallas import tpu as pltpu
from jax.sharding import PartitionSpec as P

HEAD = 128
THETA = 10000
HIDDEN = -2e30
LOG2E = 1.4426950408889634
E2 = HEAD**-0.5 * LOG2E
MESH = pl.DeviceIdType.MESH
CHIPS = 4
SLOTS = 6


def _dot(a, b, ca, cb):
    return lax.dot_general(a, b, (((ca,), (cb,)), ((), ())), preferred_element_type=jnp.float32)


def _tables(rows):
    half = HEAD // 2
    angle = np.arange(rows, dtype=np.float32)[:, None] * np.float32(THETA) ** (-np.arange(half, dtype=np.float32) / np.float32(half))
    angle = angle.astype(np.float32).astype(np.float64)
    return np.concatenate([np.cos(angle), np.sin(angle)], -1).astype(np.float32)


def _score(k, q_ref, h, s_ref, m_ref):
    s = _dot(k, q_ref[h], 1, 1)
    s_ref[...] = s
    m_ref[...] = s.max(axis=0, keepdims=True)


def _take(vt, h, s_ref, m_ref, top_s, mix_s):
    old = top_s[h]
    top = jnp.maximum(old, m_ref[...])
    top_s[h] = top
    p = jnp.exp2((s_ref[...] - top) * E2).astype(jnp.bfloat16)
    mix_s[h] = mix_s[h] * jnp.exp2((old - top) * E2) + _dot(vt, p, 1, 0)


def _score_own(k, q_ref, h, s_ref, m_ref, seen):
    half = seen.shape[0]
    low = jnp.where(seen, _dot(k[:half], q_ref[h, :half], 1, 1), HIDDEN)
    high = _dot(k, q_ref[h, half:], 1, 1)
    above, below = high[:half], jnp.where(seen, high[half:], HIDDEN)
    s_ref[:half, :half] = low
    s_ref[:half, half:] = above
    s_ref[half:, half:] = below
    m_ref[:, :half] = low.max(axis=0, keepdims=True)
    m_ref[:, half:] = jnp.maximum(above, below).max(axis=0, keepdims=True)


def _take_own(vt, h, s_ref, m_ref, top_s, mix_s):
    half = s_ref.shape[0] // 2
    top = m_ref[...]
    top_s[h] = top
    for keys, lanes in ((slice(0, half), slice(0, half)), (slice(None), slice(half, None))):
        p = jnp.exp2((s_ref[keys, lanes] - top[:, lanes]) * E2).astype(jnp.bfloat16)
        mix_s[h, :, lanes] = _dot(vt[:, keys], p, 1, 0)


def _body(x_hbm, gain_ref, wq_hbm, wk_hbm, wv_hbm, wo_hbm, tab_hbm, y_hbm, a_s, x_s, w_s, k_s, v_s, km_s, vm_s, q_s, top_s, mix_s, own_s, give_s, got_s,
          acc_s, y_s, s_s, m_s, cos_s, sin_s, x_sem, w_sem, tab_sem, xs_sem, xr_sem, mate_send, send_sem, recv_sem, fsend_sem, frecv_sem,
          swap_send, swap_recv, y_sem):
    own, depth = x_hbm.shape
    tokens = 2 * own
    kv, group = k_s.shape[1], q_s.shape[0] // k_s.shape[1]
    wide = w_s.shape[2]
    per = wide // HEAD
    qcols, kvcols = q_s.shape[0] * HEAD, kv * HEAD
    nq, nkv, pieces = qcols // wide, 4 * kvcols // wide, kv // per
    no = depth // wide
    me = lax.axis_index("sp")
    chip, core = me // 2, me % 2
    mate = chip * 2 + 1 - core
    mine = pl.ds(pl.multiple_of(core * own, own), own)

    plan = [(what, half, p) for p in range(pieces) for half in (1, 0) for what in (0, 1)]

    def kv_block(i):
        what, half, p = plan[i]
        at = pl.multiple_of(lax.rem(core + half, 2) * kvcols + p * wide, wide)
        ref = wk_hbm if what == 0 else wv_hbm
        return pltpu.make_async_copy(ref.at[:, pl.ds(at, wide)], w_s.at[i % SLOTS], w_sem.at[i % SLOTS])

    def q_block(i):
        slot = lax.rem(i + nkv, SLOTS)
        at = pl.multiple_of(core * qcols + i * wide, wide)
        return pltpu.make_async_copy(wq_hbm.at[:, pl.ds(at, wide)], w_s.at[slot], w_sem.at[slot])

    def o_block(i):
        slot = lax.rem(i + nkv + nq, SLOTS)
        rows = pl.multiple_of(jnp.where(i < no, core, 1 - core) * qcols, qcols)
        at = pl.multiple_of(lax.rem(i, no) * wide, wide)
        return pltpu.make_async_copy(wo_hbm.at[pl.ds(rows, qcols), pl.ds(at, wide)], w_s.at[slot, pl.ds(0, qcols), :], w_sem.at[slot])

    load = pltpu.make_async_copy(x_hbm, y_s, x_sem)
    load.start()
    table = pltpu.make_async_copy(tab_hbm.at[pl.ds(pl.multiple_of(chip * tokens, tokens), tokens)], cos_s, tab_sem)
    table.start()

    barrier = pltpu.get_barrier_semaphore()
    pl.semaphore_signal(barrier, inc=1, device_id={"sp": mate}, device_id_type=MESH)
    for r in (1, 2):
        for g in (0, 1):
            pl.semaphore_signal(barrier, inc=1, device_id={"sp": (chip ^ r) * 2 + g}, device_id_type=MESH)

    v_s[:, :, HEAD:, :] = jnp.ones((*v_s.shape[:2], v_s.shape[2] - HEAD, v_s.shape[3]), jnp.bfloat16)
    table.wait()
    both = cos_s[...]
    turn = pltpu.roll(both, HEAD // 2, 1)
    left = lax.broadcasted_iota(jnp.int32, both.shape, 1) < HEAD // 2
    cos_s[...] = jnp.where(left, both, turn)
    sin_s[...] = jnp.where(left, -turn, both)

    def turned(t, rows):
        t = t.astype(jnp.float32)
        return (t * cos_s[rows, :] + pltpu.roll(t, HEAD // 2, 1) * sin_s[rows, :]).astype(jnp.bfloat16)

    def normed(ref, slot, keep):
        slab = 16
        gain = gain_ref[...].reshape(1, depth).astype(jnp.float32)

        def one(i, _):
            rows = pl.ds(pl.multiple_of(i * slab, slab), slab)
            t = ref[rows, :].astype(jnp.float32)
            if keep:
                acc_s[rows, :] = t
            t = t * lax.rsqrt(jnp.mean(t * t, -1, keepdims=True) + 1e-6) * gain
            a_s[slot, rows, :] = t.astype(jnp.bfloat16)
            return 0

        lax.fori_loop(0, own // slab, one, 0, unroll=4 if keep else True)

    def places(what, half, p):
        heads = pl.ds(p * per, per)
        there = k_s.at[chip, heads, mine, :] if what == 0 else v_s.at[chip, heads, pl.ds(0, HEAD), mine]
        if half == 0:
            return there, there
        return (km_s if what == 0 else vm_s).at[heads], there

    def to_mate(what, p):
        src, dst = places(what, 1, p)
        return pltpu.make_async_remote_copy(src_ref=src, dst_ref=dst, send_sem=mate_send.at[what, p], recv_sem=recv_sem.at[chip, core, what, p],
                                            device_id={"sp": mate}, device_id_type=MESH)

    def to_chip(r, what, half, p):
        src, dst = places(what, half, p)
        return pltpu.make_async_remote_copy(src_ref=src, dst_ref=dst, send_sem=send_sem.at[r, what, half, p],
                                            recv_sem=recv_sem.at[chip, core, what, p],
                                            device_id={"sp": (chip ^ r) * 2 + lax.rem(core + half, 2)}, device_id_type=MESH)

    def arrived(there, by, what, p):
        heads, rows = pl.ds(p * per, per), pl.ds(pl.multiple_of(by * own, own), own)
        ref = k_s.at[there, heads, rows, :] if what == 0 else v_s.at[there, heads, pl.ds(0, HEAD), rows]
        pltpu.make_async_remote_copy(src_ref=ref, dst_ref=ref, send_sem=mate_send.at[what, p], recv_sem=recv_sem.at[there, by, what, p],
                                     device_id={"sp": mate}, device_id_type=MESH).wait_recv()

    def passed(source, target, what, p):
        heads = pl.ds(p * per, per)
        ref = k_s.at[source, heads] if what == 0 else v_s.at[source, heads, pl.ds(0, HEAD), :]
        return pltpu.make_async_remote_copy(src_ref=ref, dst_ref=ref, send_sem=fsend_sem.at[what, p], recv_sem=frecv_sem.at[what, p],
                                            device_id={"sp": target * 2 + core}, device_id_type=MESH)

    source = jnp.where((chip == 0) | (chip == 3), 1, 0)

    def takes(r, what):
        later = (chip ^ r) > chip
        return later | (chip == r) if (r, what) == (1, 0) else later

    def from_near(p):
        for r in (1, 2):
            for what in (0, 1):
                near = (chip ^ r) < chip

                @pl.when(near | (chip == 0) if (r, what) == (1, 0) else near)
                def _():
                    arrived(chip ^ r, 0, what, p)
                    arrived(chip ^ r, 1, what, p)
        for what in (0, 1):
            @pl.when(chip // 2 == what)
            def _():
                passed(source, 3 - source, what, p).start()

    def send(i):
        for what, half, p in plan[i : i + 2]:
            if half:
                to_mate(what, p).start()
            for r in (1, 2):
                @pl.when(takes(r, what))
                def _():
                    to_chip(r, what, half, p).start()

    load.wait()
    for i in range(SLOTS):
        kv_block(i).start()
    normed(y_s, core, True)
    pl.semaphore_wait(barrier, 5)

    give = pltpu.make_async_remote_copy(src_ref=x_hbm, dst_ref=x_s, send_sem=xs_sem, recv_sem=xr_sem, device_id={"sp": mate},
                                        device_id_type=MESH)
    give.start()

    for i in range(0, nkv, 2):
        for m in (i, i + 1):
            kv_block(m).wait()
        if i:
            send(i - 2)
        if i == nkv - 2:
            give.wait_recv()
            normed(x_s, 1 - core, False)
        for m in (i, i + 1):
            what, half, p = plan[m]
            t = _dot(a_s[core], w_s[m % SLOTS], 1, 0)
            for j in range(per):
                u = t[:, j * HEAD : (j + 1) * HEAD]
                n = p * per + j
                if what == 0:
                    u = turned(u.astype(jnp.bfloat16), mine)
                    if half:
                        km_s[n] = u
                    else:
                        k_s[chip, n, mine, :] = u
                else:
                    u = u.astype(jnp.bfloat16).T
                    if half:
                        vm_s[n] = u
                    else:
                        v_s[chip, n, :HEAD, mine] = u
        for m in (i + SLOTS, i + 1 + SLOTS):
            if m < nkv:
                kv_block(m).start()
            else:
                q_block(m - nkv).start()
    send(nkv - 2)

    def project(trip, _):
        for j in range(3):
            q_block(3 * trip + j).wait()
        for j in range(3):
            i = 3 * trip + j
            t = _dot(a_s[...].reshape(tokens, depth), w_s[lax.rem(i + nkv, SLOTS)], 1, 0).astype(jnp.bfloat16)
            for m in range(per):
                q_s[i * per + m] = turned(t[:, m * HEAD : (m + 1) * HEAD], slice(None))
        for j in range(3):
            i = 3 * trip + j + SLOTS

            @pl.when(i < nq)
            def _():
                q_block(i).start()

            @pl.when(i >= nq)
            def _():
                o_block(i - nq).start()
        return 0

    lax.fori_loop(0, nq // 3, project, 0)
    from_near(0)

    for p in range(pieces):
        for what in (0, 1):
            arrived(chip, 1 - core, what, p)

    part = group // 2
    seen = lax.broadcasted_iota(jnp.int32, (own, own), 1) >= lax.broadcasted_iota(jnp.int32, (own, own), 0)

    def staged(score, take, now, later):
        order = [(now, 0), (now, part), (now + 1, 0), (now + 1, part), (later, 0)]
        for i in range(4):
            (n, at), (ahead, to) = order[i], order[i + 1]
            for j in range(part):
                score(ahead, to + j, s_s.at[(i + 1) % 2, j], m_s.at[(i + 1) % 2, j])
                take(n, at + j, s_s.at[i % 2, j], m_s.at[i % 2, j])
        return 0

    def own_score(n, j, s_ref, m_ref):
        _score_own(k_s[chip, n], q_s, n * group + j, s_ref, m_ref, seen)

    def own_take(n, j, s_ref, m_ref):
        _take_own(v_s[chip, n], n * group + j, s_ref, m_ref, top_s, mix_s)

    for j in range(part):
        own_score(0, j, s_s.at[0, j], m_s.at[0, j])
    lax.fori_loop(0, kv // 2, lambda i, _: staged(own_score, own_take, 2 * i, jnp.minimum(2 * i + 2, kv - 1)), 0)

    @pl.when(chip < 3)
    def _():
        from_near(1)

    @pl.when(chip > 0)
    def _():
        last = chip * kv - 1

        def chunk(t):
            return chip ^ (lax.div(t, kv) + jnp.where(chip == 2, 2, 1)), lax.rem(t, kv)

        def more_score(t, j, s_ref, m_ref):
            there, n = chunk(t)
            _score(k_s[there, n], q_s, n * group + j, s_ref, m_ref)

        def more_take(t, j, s_ref, m_ref):
            there, n = chunk(t)
            _take(v_s[there, n], n * group + j, s_ref, m_ref, top_s, mix_s)

        def more(i, _):
            t = 2 * i
            @pl.when((chip == 3) & (t == 0))
            def _():
                from_near(1)

            for p in range(pieces):
                @pl.when((t + 1 + kv == last + p * per) & (chip >= 2))
                def _():
                    for what in (0, 1):
                        passed(chip ^ 3, chip, what, p).wait_recv()

            return staged(more_score, more_take, t, jnp.minimum(t + 2, last))

        for j in range(part):
            more_score(0, j, s_s.at[0, j], m_s.at[0, j])
        lax.fori_loop(0, (last + 1) // 2, more, 0)

    def swap(n):
        columns = pl.ds(pl.multiple_of(n * group * HEAD, HEAD), group * HEAD)
        return pltpu.make_async_remote_copy(src_ref=give_s.at[:, columns], dst_ref=got_s.at[:, columns], send_sem=swap_send.at[n],
                                            recv_sem=swap_recv.at[n], device_id={"sp": mate}, device_id_type=MESH)

    def finish(n, _):
        for j in range(group):
            h = n * group + j
            column = pl.ds(pl.multiple_of(h * HEAD, HEAD), HEAD)
            for part, ref in ((core, own_s), (1 - core, give_s)):
                lanes = pl.ds(pl.multiple_of(part * own, own), own)
                t = mix_s[h, :HEAD, lanes] * (1 / mix_s[h, HEAD : HEAD + 1, lanes])
                ref[:, column] = t.astype(jnp.bfloat16).T

        @pl.when(n > 0)
        def _():
            swap(n - 1).start()
        return 0

    lax.fori_loop(0, kv, finish, 0)

    def out(trip, second):
        for j in (0, 1):
            o_block(2 * trip + j).wait()
        for j in (0, 1):
            i = 2 * trip + j
            column = pl.ds(pl.multiple_of(lax.rem(i, no) * wide, wide), wide)
            t = acc_s[:, column] + _dot((got_s if second else own_s)[...], w_s[lax.rem(i + nkv + nq, SLOTS), :qcols, :], 1, 0)
            if second:
                y_s[:, column] = t.astype(jnp.bfloat16)
            else:
                acc_s[:, column] = t
        for j in (0, 1):
            i = 2 * trip + j + SLOTS

            @pl.when(i < 2 * no)
            def _():
                o_block(i).start()

    def result(i):
        column = pl.ds(pl.multiple_of(i * 2 * wide, wide), 2 * wide)
        return pltpu.make_async_copy(y_s.at[:, column], y_hbm.at[:, column], y_sem.at[i])

    def out_own(trip, _):
        out(trip, False)

        @pl.when(trip == 0)
        def _():
            swap(kv - 1).start()
        return 0

    lax.fori_loop(0, no // 2, out_own, 0)
    for n in range(kv):
        swap(n).wait_recv()

    def out_mate(trip, _):
        out(trip, True)

        @pl.when(trip > no // 2)
        def _():
            result(trip - no // 2 - 1).start()
        return 0

    lax.fori_loop(no // 2, no, out_mate, 0)
    result(no // 2 - 1).start()

    for p in range(pieces):
        for what in (0, 1):
            to_mate(what, p).wait_send()
    for r in (1, 2):
        for what in (0, 1):
            @pl.when(takes(r, what))
            def _():
                for p in range(pieces):
                    for half in (0, 1):
                        to_chip(r, what, half, p).wait_send()
    for what in (0, 1):
        @pl.when(chip // 2 == what)
        def _():
            for p in range(pieces):
                passed(source, 3 - source, what, p).wait_send()
    for n in range(kv):
        swap(n).wait_send()
    give.wait_send()
    for i in range(no // 2):
        result(i).wait()


def _program(x, gain, wq, wk, wv, wo):
    own, depth = x.shape
    tokens, heads, kv = 2 * own, wq.shape[1] // HEAD // 2, wk.shape[1] // HEAD // 2
    wide, bf, f32 = 256, jnp.bfloat16, jnp.float32
    table = jnp.asarray(_tables(tokens * CHIPS))
    hbm = pl.BlockSpec(memory_space=pl.ANY)
    dma = pltpu.SemaphoreType.DMA
    return pl.pallas_call(
        _body,
        out_shape=jax.ShapeDtypeStruct((own, depth), bf),
        in_specs=[hbm, pl.BlockSpec(memory_space=pltpu.VMEM), hbm, hbm, hbm, hbm, hbm],
        out_specs=hbm,
        scratch_shapes=[
            pltpu.VMEM((2, own, depth), bf),
            pltpu.VMEM((own, depth), bf),
            pltpu.VMEM((SLOTS, depth, wide), bf),
            pltpu.VMEM((CHIPS, kv, tokens, HEAD), bf),
            pltpu.VMEM((CHIPS, kv, HEAD + 16, tokens), bf),
            pltpu.VMEM((kv, own, HEAD), bf),
            pltpu.VMEM((kv, HEAD, own), bf),
            pltpu.VMEM((heads, tokens, HEAD), bf),
            pltpu.VMEM((heads, 1, tokens), f32),
            pltpu.VMEM((heads, HEAD + 16, tokens), f32),
            pltpu.VMEM((own, heads * HEAD), bf),
            pltpu.VMEM((own, heads * HEAD), bf),
            pltpu.VMEM((own, heads * HEAD), bf),
            pltpu.VMEM((own, depth), f32),
            pltpu.VMEM((own, depth), bf),
            pltpu.VMEM((2, heads // kv // 2, tokens, tokens), f32),
            pltpu.VMEM((2, heads // kv // 2, 1, tokens), f32),
            pltpu.VMEM((tokens, HEAD), f32),
            pltpu.VMEM((tokens, HEAD), f32),
            dma, dma((SLOTS,)), dma, dma, dma, dma((2, 2)), dma((3, 2, 2, 2)), dma((CHIPS, 2, 2, 2)), dma((2, 2)), dma((2, 2)),
            dma((kv,)), dma((kv,)), dma((depth // wide // 2,)),
        ],
        compiler_params=pltpu.CompilerParams(collective_id=0, has_side_effects=True, vmem_limit_bytes=67043328),
        name="layer",
    )(x, gain, wq, wk, wv, wo, table)


def _copy_body(x_hbm, y_hbm, buf, in_sem, out_sem):
    parts, rows = buf.shape[:2]

    def take(i):
        return pltpu.make_async_copy(x_hbm.at[pl.ds(i * rows, rows)], buf.at[i], in_sem.at[i])

    def put(i):
        return pltpu.make_async_copy(buf.at[i], y_hbm.at[pl.ds(i * rows, rows)], out_sem.at[i])

    for i in range(parts):
        take(i).start()
    for i in range(parts):
        take(i).wait()
        put(i).start()
    for i in range(parts):
        put(i).wait()


def _copied(x, parts=8):
    hbm, dma = pl.BlockSpec(memory_space=pl.ANY), pltpu.SemaphoreType.DMA
    return pl.pallas_call(
        _copy_body,
        out_shape=jax.ShapeDtypeStruct(x.shape, x.dtype),
        in_specs=[hbm],
        out_specs=hbm,
        scratch_shapes=[pltpu.VMEM((parts, x.shape[0] // parts, x.shape[1]), x.dtype), dma((parts,)), dma((parts,))],
        compiler_params=pltpu.CompilerParams(vmem_limit_bytes=67043328),
        name="copied",
    )(x)


def solution(mesh):
    tokens, whole = P(("dp", "sp"), None), P(None, None)
    return jax.shard_map(
        lambda *args: _copied(_program(*args)),
        mesh=mesh,
        in_specs=(tokens, P(None), whole, whole, whole, whole),
        out_specs=tokens,
        check_vma=False,
    )
```
